32 devices in a mesh: seq: 8 (over z, x), head: 4 (over y, core).
Axes of the slice: x: 2, y: 2, z: 4, core: 2. Of those that a mesh axis runs over, the one named last changes fastest.
Arguments:
- block_input: float32 [1, 2048, 1536], P(None, 'seq'), may hold values from -6 to 6
- cotangent: float32 [1, 2048, 1536], P(None, 'seq'), may hold values from -6 to 6
- gate_proj: float32 [1536, 3072], P('seq', 'head'), may hold values from -0.15625 to 0.15625
- value_proj: float32 [1536, 3072], P('seq', 'head'), may hold values from -0.15625 to 0.15625
- bc_proj: float32 [1536, 256], P('seq'), may hold values from -0.15625 to 0.15625
- step_proj: float32 [1536, 48], P('seq', 'head'), may hold values from -0.15625 to 0.15625
- out_proj: float32 [3072, 1536], P('head', 'seq'), may hold values from -0.109375 to 0.109375
- in_gain: float32 [1536], replicated, may hold values from 0.5 to 1.5
- conv_value: float32 [5, 3072], replicated, may hold values from -3 to 3
- conv_bc: float32 [5, 256], replicated, may hold values from -3 to 3
- head_params: float32 [3, 48], replicated, as said below
- out_gain: float32 [3072], replicated, may hold values from 0.5 to 1.5
- m_gate: float32 [1536, 3072], P('seq', 'head'), may hold values from -24 to 24
- m_value: float32 [1536, 3072], P('seq', 'head'), may hold values from -24 to 24
- m_bc: float32 [1536, 256], P('seq'), may hold values from -24 to 24
- m_step: float32 [1536, 48], P('seq', 'head'), may hold values from -24 to 24
- m_out: float32 [3072, 1536], P('head', 'seq'), may hold values from -24 to 24
- m_ingain: float32 [1536], replicated, may hold values from -6 to 6
- m_convvalue: float32 [5, 3072], replicated, may hold values from -6 to 6
- m_convbc: float32 [5, 256], replicated, may hold values from -6 to 6
- m_head: float32 [3, 48], replicated, may hold values from -6 to 6
- m_outgain: float32 [3072], replicated, may hold values from -6 to 6
Outputs:
- block_output: float32 [1, 2048, 1536], P(None, 'seq', 'head')
- input_grad: float32 [1, 2048, 1536], P(None, 'seq', 'head')
- grad_gate: float32 [1536, 3072], P('seq', 'head')
- grad_value: float32 [1536, 3072], P('seq', 'head')
- grad_bc: float32 [1536, 256], P('seq')
- grad_step: float32 [1536, 48], P('seq', 'head')
- grad_out: float32 [3072, 1536], P('head', 'seq')
- grad_ingain: float32 [1536], replicated
- grad_convvalue: float32 [5, 3072], replicated
- grad_convbc: float32 [5, 256], replicated
- grad_head: float32 [3, 48], replicated
- grad_outgain: float32 [3072], replicated
- new_gate: float32 [1536, 3072], P('seq', 'head')
- new_value: float32 [1536, 3072], P('seq', 'head')
- new_bc: float32 [1536, 256], P('seq')
- new_step: float32 [1536, 48], P('seq', 'head')
- new_out: float32 [3072, 1536], P('head', 'seq')
- new_ingain: float32 [1536], replicated
- new_convvalue: float32 [5, 3072], replicated
- new_convbc: float32 [5, 256], replicated
- new_head: float32 [3, 48], replicated
- new_outgain: float32 [3072], replicated
- next_gate: float32 [1536, 3072], P('seq', 'head')
- next_value: float32 [1536, 3072], P('seq', 'head')
- next_bc: float32 [1536, 256], P('seq')
- next_step: float32 [1536, 48], P('seq', 'head')
- next_out: float32 [3072, 1536], P('head', 'seq')
- next_ingain: float32 [1536], replicated
- next_convvalue: float32 [5, 3072], replicated
- next_convbc: float32 [5, 256], replicated
- next_head: float32 [3, 48], replicated
- next_outgain: float32 [3072], replicated
The draws below stay inside these ranges and needn't reach their ends.
Inputs may be any that keep to these rules, and one draw needn't show every extreme that they name: `head_params`: row 0 is each head's logarithm of its decay rate, row 1 its skip gain, row 2 the bias of its step size.
All inputs are finite; a program needn't handle non-finite values.
Results may differ from the reference program's by a relative error of at most 0.0003.
Values sent between devices are 32-bit elements; how exact they have to be, the bound alone decides.
A program may use at most 192 MiB of HBM per device.

```python
import math
import jax
import jax.numpy as jnp
from jax import lax

D = 1536
DI = 3072
STATE = 128
HEADDIM = 64
H = 48
GROUP = 256
CONV = 4
SWEEPS = 5
SEQS = 1
LEN = 2048
N_HEAD = 4


def draw_head_params(key, part):
    subkeys = jax.random.split(jax.random.fold_in(key, 11), 3)
    a_log = jax.random.uniform(subkeys[0], (H,), jnp.float32, 0.0, 2.8)
    skip_gain = jax.random.uniform(subkeys[1], (H,), jnp.float32, 0.5, 1.5)
    log_rate = jax.random.uniform(subkeys[2], (H,), jnp.float32, math.log(0.5 / LEN), math.log(0.05))
    step_bias = log_rate - a_log - 0.5
    return jnp.stack([a_log, skip_gain, step_bias]).astype(jnp.float32)


def block_levels(stream_key, shape, cuts, smallest, top_value):
    level = 1.0
    for axis_at, blocks in cuts:
        draws = jax.random.uniform(jax.random.fold_in(jax.random.fold_in(stream_key, 6), axis_at), (blocks,), jnp.float32, smallest / len(cuts), top_value / len(cuts))
        level = level * jnp.repeat(jnp.exp(draws), shape[axis_at] // blocks).reshape((-1,) + (1,) * (len(shape) - 1 - axis_at))
    return level


def scatter_about(key, shape, deviation, reach, cuts=(), kind=jnp.bfloat16):
    values = deviation * jax.random.normal(key, shape, jnp.float32)
    if cuts:
        values = values * block_levels(key, shape, cuts, -0.22, 0.18)
    return jnp.clip(values, -reach, reach).astype(kind)


def setup_inputs(seed: int = 0) -> dict:
    seeds = jax.random.split(jax.random.key(seed), 23)
    block_input = scatter_about(seeds[0], (SEQS, LEN, D), 1.0, 6.0, ((1, 8),), jnp.float32)
    cotangent = scatter_about(seeds[1], (SEQS, LEN, D), 1.0, 6.0, ((1, 8),), jnp.float32)
    gate_proj = scatter_about(seeds[2], (D, DI), D ** -0.5, 0.15625, ((0, 8), (1, 4)), jnp.float32)
    value_proj = scatter_about(seeds[3], (D, DI), D ** -0.5, 0.15625, ((0, 8), (1, 4)), jnp.float32)
    bc_proj = scatter_about(seeds[4], (D, 2 * STATE), D ** -0.5, 0.15625, ((0, 8),), jnp.float32)
    step_proj = scatter_about(seeds[5], (D, H), D ** -0.5, 0.15625, ((0, 8), (1, 4)), jnp.float32)
    out_proj = scatter_about(seeds[6], (DI, D), DI ** -0.5, 0.109375, ((0, 4), (1, 8)), jnp.float32)
    in_gain = jnp.clip(1.0 + 0.1 * jax.random.normal(seeds[7], (D,), jnp.float32), 0.5, 1.5)
    conv_value = scatter_about(seeds[8], (CONV + 1, DI), 0.5, 3.0, (), jnp.float32)
    conv_bc = scatter_about(seeds[9], (CONV + 1, 2 * STATE), 0.5, 3.0, (), jnp.float32)
    head_params = draw_head_params(jax.random.fold_in(seeds[22], 71), 0)
    out_gain = jnp.clip(1.0 + 0.1 * jax.random.normal(seeds[11], (DI,), jnp.float32), 0.5, 1.5)
    m_gate = scatter_about(seeds[12], (D, DI), 4.0, 24.0, ((0, 8), (1, 4)), jnp.float32)
    m_value = scatter_about(seeds[13], (D, DI), 4.0, 24.0, ((0, 8), (1, 4)), jnp.float32)
    m_bc = scatter_about(seeds[14], (D, 2 * STATE), 4.0, 24.0, ((0, 8),), jnp.float32)
    m_step = scatter_about(seeds[15], (D, H), 4.0, 24.0, ((0, 8), (1, 4)), jnp.float32)
    m_out = scatter_about(seeds[16], (DI, D), 4.0, 24.0, ((0, 4), (1, 8)), jnp.float32)
    m_ingain = scatter_about(seeds[17], (D,), 1.0, 6.0, (), jnp.float32)
    m_convvalue = scatter_about(seeds[18], (CONV + 1, DI), 1.0, 6.0, (), jnp.float32)
    m_convbc = scatter_about(seeds[19], (CONV + 1, 2 * STATE), 1.0, 6.0, (), jnp.float32)
    m_head = scatter_about(seeds[20], (3, H), 1.0, 6.0, (), jnp.float32)
    m_outgain = scatter_about(seeds[21], (DI,), 1.0, 6.0, (), jnp.float32)
    return {"block_input": block_input, "cotangent": cotangent, "gate_proj": gate_proj, "value_proj": value_proj, "bc_proj": bc_proj, "step_proj": step_proj, "out_proj": out_proj, "in_gain": in_gain, "conv_value": conv_value, "conv_bc": conv_bc, "head_params": head_params, "out_gain": out_gain, "m_gate": m_gate, "m_value": m_value, "m_bc": m_bc, "m_step": m_step, "m_out": m_out, "m_ingain": m_ingain, "m_convvalue": m_convvalue, "m_convbc": m_convbc, "m_head": m_head, "m_outgain": m_outgain}


HIGHEST = lax.Precision.HIGHEST
EPSILON = 1e-05
QUINTIC_A = 3.4445
QUINTIC_B = -4.775
QUINTIC_C = 2.0315
MOMENTUM_KEEP = 0.9
MATRIX_RATE = 0.02
VECTOR_RATE = 0.002
MUON_SCALE = 0.2

def project(activation, weight):
    return jnp.einsum('std,dk->stk', activation, weight, precision=HIGHEST)

def mixer_scan(values, step_size, log_decay, b_state, c_state, skip_gain):
    seq_count, length, width = values.shape
    blocks = length // GROUP
    rows_at = lax.broadcasted_iota(jnp.int32, (GROUP, GROUP), 0)
    cols_at = lax.broadcasted_iota(jnp.int32, (GROUP, GROUP), 1)
    lower_mask = rows_at >= cols_at
    lower_ones = lower_mask.astype(jnp.float32)

    def to_blocks(array):
        return array.reshape((seq_count, blocks, GROUP) + array.shape[2:]).swapaxes(0, 1)

    def group_step(carried, pieces):
        head_values, step_blocks, decay_blocks, b_blocks, c_blocks = pieces
        within = jnp.einsum('ij,sjh->sih', lower_ones, decay_blocks, precision=HIGHEST)
        decay_rows = within.transpose(0, 2, 1)
        log_gaps = decay_rows[:, :, :, None] - decay_rows[:, :, None, :]
        decay_mat = jnp.where(lower_mask, jnp.exp(jnp.where(lower_mask, log_gaps, 0.0)), 0.0)
        scores = jnp.einsum('sin,sjn->sij', c_blocks, b_blocks, precision=HIGHEST)
        weighted = scores[:, None] * decay_mat * step_blocks.transpose(0, 2, 1)[:, :, None, :]
        intra_out = jnp.einsum('shij,sjhp->sihp', weighted, head_values, precision=HIGHEST)
        inter_out = jnp.einsum('sin,shpn->sihp', c_blocks, carried, precision=HIGHEST) * jnp.exp(within)[..., None]
        result = intra_out + inter_out + skip_gain[:, None] * head_values
        to_end = jnp.exp(within[:, -1:, :] - within) * step_blocks
        fresh = jnp.einsum('sjh,sjhp,sjn->shpn', to_end, head_values, b_blocks, precision=HIGHEST)
        updated = jnp.exp(within[:, -1, :])[..., None, None] * carried + fresh
        return (updated, result)
    start_state = jnp.zeros((seq_count, H, HEADDIM, STATE), jnp.float32)
    head_values = values.reshape(seq_count, length, H, HEADDIM)
    _, outputs = lax.scan(group_step, start_state, (to_blocks(head_values), to_blocks(step_size), to_blocks(log_decay), to_blocks(b_state), to_blocks(c_state)))
    return outputs.swapaxes(0, 1).reshape(seq_count, length, width)

def layer_forward(block_input, gate_proj, value_proj, bc_proj, step_proj, out_proj, in_gain, conv_value, conv_bc, head_params, out_gain):
    length = block_input.shape[1]
    inv_rms = lax.rsqrt(lax.optimization_barrier(jnp.mean(block_input * block_input, axis=-1, keepdims=True)) + EPSILON)
    normed = block_input * inv_rms * in_gain
    gate_pre = project(normed, gate_proj)
    mixed_pre = project(normed, jnp.concatenate([value_proj, bc_proj], axis=1))
    step_pre = project(normed, step_proj)
    conv_taps = jnp.concatenate([conv_value, conv_bc], axis=1)
    padded = jnp.pad(mixed_pre, ((0, 0), (CONV - 1, 0), (0, 0)))
    conv_out = conv_taps[CONV] + sum((conv_taps[offset] * padded[:, offset:offset + length, :] for offset in range(CONV)))
    activated = jax.nn.silu(conv_out)
    values = activated[..., :DI]
    b_state = activated[..., DI:DI + STATE]
    c_state = activated[..., DI + STATE:]
    step_size = jax.nn.softplus(step_pre + head_params[2])
    log_decay = -jnp.exp(head_params[0]) * step_size
    mixer_out = mixer_scan(values, step_size, log_decay, b_state, c_state, head_params[1])
    gated = mixer_out * jax.nn.silu(gate_pre)
    gate_rms = lax.rsqrt(lax.optimization_barrier(jnp.mean(gated * gated, axis=-1, keepdims=True)) + EPSILON)
    return block_input + project(gated * gate_rms * out_gain, out_proj)

def orthogonalize(matrix):
    current = matrix / (jnp.sqrt(jnp.sum(matrix * matrix)) + 1e-07)
    for iteration in range(SWEEPS):
        gramian = jnp.dot(current, current.T, precision=HIGHEST)
        current = QUINTIC_A * current + jnp.dot(QUINTIC_B * gramian + QUINTIC_C * jnp.dot(gramian, gramian, precision=HIGHEST), current, precision=HIGHEST)
    return current

def column_blocks(matrix):
    width = matrix.shape[1] // N_HEAD
    return jnp.concatenate([orthogonalize(matrix[:, index * width:(index + 1) * width].T).T for index in range(N_HEAD)], axis=1)

def row_blocks(matrix):
    height = matrix.shape[0] // N_HEAD
    return jnp.concatenate([orthogonalize(matrix[index * height:(index + 1) * height, :]) for index in range(N_HEAD)], axis=0)

def reference(block_input, cotangent, gate_proj, value_proj, bc_proj, step_proj, out_proj, in_gain, conv_value, conv_bc, head_params, out_gain, m_gate, m_value, m_bc, m_step, m_out, m_ingain, m_convvalue, m_convbc, m_head, m_outgain):
    weights = (gate_proj, value_proj, bc_proj, step_proj, out_proj, in_gain, conv_value, conv_bc, head_params, out_gain)
    block_output, pullback = jax.vjp(layer_forward, block_input, *weights)
    gradients = pullback(cotangent)
    input_grad = gradients[0]
    grad_gate, grad_value, grad_bc, grad_step, grad_out, grad_ingain, grad_convvalue, grad_convbc, grad_head, grad_outgain = gradients[1:]
    next_gate = MOMENTUM_KEEP * m_gate + grad_gate
    next_value = MOMENTUM_KEEP * m_value + grad_value
    next_bc = MOMENTUM_KEEP * m_bc + grad_bc
    next_step = MOMENTUM_KEEP * m_step + grad_step
    next_out = MOMENTUM_KEEP * m_out + grad_out
    next_ingain = MOMENTUM_KEEP * m_ingain + grad_ingain
    next_convvalue = MOMENTUM_KEEP * m_convvalue + grad_convvalue
    next_convbc = MOMENTUM_KEEP * m_convbc + grad_convbc
    next_head = MOMENTUM_KEEP * m_head + grad_head
    next_outgain = MOMENTUM_KEEP * m_outgain + grad_outgain
    update_scale = MATRIX_RATE * MUON_SCALE * D ** 0.5
    new_gate = gate_proj - update_scale * column_blocks(next_gate)
    new_value = value_proj - update_scale * column_blocks(next_value)
    new_bc = bc_proj - update_scale * orthogonalize(next_bc.T).T
    new_step = step_proj - update_scale * column_blocks(next_step)
    new_out = out_proj - update_scale * row_blocks(next_out)
    new_ingain = in_gain - VECTOR_RATE * next_ingain
    new_convvalue = conv_value - VECTOR_RATE * next_convvalue
    new_convbc = conv_bc - VECTOR_RATE * next_convbc
    new_head = head_params - VECTOR_RATE * next_head
    new_outgain = out_gain - VECTOR_RATE * next_outgain
    return (block_output, input_grad, grad_gate, grad_value, grad_bc, grad_step, grad_out, grad_ingain, grad_convvalue, grad_convbc, grad_head, grad_outgain, new_gate, new_value, new_bc, new_step, new_out, new_ingain, new_convvalue, new_convbc, new_head, new_outgain, next_gate, next_value, next_bc, next_step, next_out, next_ingain, next_convvalue, next_convbc, next_head, next_outgain)
```

```python
import math

import jax
import jax.numpy as jnp
from jax import lax
from jax.sharding import PartitionSpec as P

D = 1536
DI = 3072
STATE = 128
H = 48
GROUP = 256
CONV = 4
SWEEPS = 5


PRECISE = lax.Precision.HIGH
EPSILON = 1e-05
QUINTIC_A = 3.4445
QUINTIC_B = -4.775
QUINTIC_C = 2.0315
MOMENTUM_KEEP = 0.9
MATRIX_RATE = 0.02
VECTOR_RATE = 0.002
MUON_SCALE = 0.2


LANES = 128


def from_behind(value, axis, steps):
    count = lax.axis_size(axis)
    initial, last = (max(0, -steps), min(count, count - steps))
    return lax.ppermute(value, axis, [(source, source + steps) for source in range(initial, last)])


def silu_grad(pre_value):
    sigmoid_val = jax.nn.sigmoid(pre_value)
    return sigmoid_val * (1.0 + pre_value * (1.0 - sigmoid_val))


def project(activation, weight):
    return jnp.einsum("std,dk->stk", activation, weight, precision=PRECISE)


def back_project(upstream, weight):
    return jnp.einsum("stk,dk->std", upstream, weight, precision=PRECISE)


def weight_grad(activation, upstream):
    return jnp.einsum("std,stk->dk", activation, upstream, precision=PRECISE)


def place_slice(portion, full_size, offset, along):
    full_shape = list(portion.shape)
    full_shape[along] = full_size
    return lax.dynamic_update_slice_in_dim(
        jnp.zeros(full_shape, jnp.float32), portion, offset, along
    )


def running_decay(log_decay):
    seq_count, tokens, head_count = log_decay.shape
    blocks = tokens // GROUP
    grouped = log_decay.reshape(seq_count, blocks, GROUP, head_count)
    rows_at = lax.broadcasted_iota(jnp.int32, (GROUP, GROUP), 0)
    cols_at = lax.broadcasted_iota(jnp.int32, (GROUP, GROUP), 1)
    lower_mask = rows_at >= cols_at
    within = jnp.einsum("ij,sbjh->sbih", lower_mask.astype(jnp.float32), grouped, precision=PRECISE)
    group_total = within[:, :, -1, :]
    through = jnp.cumsum(group_total, axis=1)
    before = through - group_total
    return (lower_mask, within, group_total, through, before)


def group_core(values, step_size, log_decay, b_state, c_state, skip_gain):
    seq_count, tokens, width = values.shape
    head_count = step_size.shape[2]
    head_dim = width // head_count
    blocks = tokens // GROUP
    lower_mask, within, group_total, through, before = running_decay(log_decay)
    head_values = values.reshape(seq_count, blocks, GROUP, head_count, head_dim)
    step_blocks = step_size.reshape(seq_count, blocks, GROUP, head_count)
    b_blocks = b_state.reshape(seq_count, blocks, GROUP, -1)
    c_blocks = c_state.reshape(seq_count, blocks, GROUP, -1)
    decay_rows = within.transpose(0, 1, 3, 2)
    log_gaps = decay_rows[..., :, None] - decay_rows[..., None, :]
    decay_mat = jnp.where(lower_mask, jnp.exp(jnp.where(lower_mask, log_gaps, 0.0)), 0.0)
    scores = jnp.einsum("sbin,sbjn->sbij", c_blocks, b_blocks, precision=PRECISE)
    weighted = scores[:, :, None] * decay_mat * step_blocks.transpose(0, 1, 3, 2)[:, :, :, None, :]
    intra_out = jnp.einsum("sbhij,sbjhp->sbihp", weighted, head_values, precision=PRECISE)
    to_end = jnp.exp(group_total[:, :, None, :] - within) * step_blocks
    states = jnp.einsum("sbjh,sbjhp,sbjn->sbhpn", to_end, head_values, b_blocks, precision=PRECISE)
    later_at = lax.broadcasted_iota(jnp.int32, (blocks, blocks), 0)
    earlier_at = lax.broadcasted_iota(jnp.int32, (blocks, blocks), 1)
    earlier_mask = (later_at > earlier_at)[None, :, :, None]
    carry_gap = before[:, :, None, :] - through[:, None, :, :]
    carry_factor = jnp.where(earlier_mask, jnp.exp(jnp.where(earlier_mask, carry_gap, 0.0)), 0.0)
    entering = jnp.einsum("skmh,smhpn->skhpn", carry_factor, states, precision=PRECISE)
    inter_out = (
        jnp.einsum("sbin,sbhpn->sbihp", c_blocks, entering, precision=PRECISE)
        * jnp.exp(within)[..., None]
    )
    output = intra_out + inter_out + skip_gain[:, None] * head_values
    end_gap = through - through
    summary = jnp.einsum("sbh,sbhpn->shpn", jnp.exp(end_gap), states, precision=PRECISE)
    decay_all = jnp.exp(through[:, -1, :])
    return (output.reshape(seq_count, tokens, width), decay_all, summary)


def entry_term(entry_state, log_decay, c_state):
    seq_count, tokens, head_count = log_decay.shape
    blocks = tokens // GROUP
    _, within, _, _, before = running_decay(log_decay)
    reach = jnp.exp(within + before[:, :, None, :])
    c_blocks = c_state.reshape(seq_count, blocks, GROUP, -1)
    result = (
        jnp.einsum("sbin,shpn->sbihp", c_blocks, entry_state, precision=PRECISE) * reach[..., None]
    )
    return result.reshape(seq_count, tokens, -1)


def full_mixer(values, step_size, log_decay, b_state, c_state, skip_gain, entry_state):
    base_out, decay_all, summary = group_core(
        values, step_size, log_decay, b_state, c_state, skip_gain
    )
    output = base_out + entry_term(entry_state, log_decay, c_state)
    leaving = decay_all[..., None, None] * entry_state + summary
    return (output, leaving)


def gather_states(states, totals, axis):
    heads, dims, width = states.shape
    rows = states.reshape(heads * dims, width)
    if totals is not None:
        extra = jnp.pad(totals[None, :], ((0, 7), (0, width - heads)))
        rows = jnp.concatenate([rows, extra], axis=0)
    gathered = lax.all_gather(rows, axis)
    states = gathered[:, : heads * dims].reshape(-1, heads, dims, width)
    return states, None if totals is None else gathered[:, heads * dims, :heads]


def carried_states(gathered, totals, axis, reverse):
    count = lax.axis_size(axis)
    place = lax.axis_index(axis)
    at = jnp.arange(count)
    source, middle = at[:, None], at[None, :]
    if reverse:
        between = (middle > place) & (middle < source)
        used = at > place
    else:
        between = (middle < place) & (middle > source)
        used = at < place
    gap = jnp.sum(jnp.where(between[:, :, None], totals[None, :, :], 0.0), axis=1)
    factor = jnp.where(used[:, None], jnp.exp(gap), 0.0)
    return jnp.sum(factor[:, :, None, None] * gathered, axis=0)


def pack_symmetric(square):
    size = square.shape[0]
    blocks = size // LANES
    packed = []
    for first in range(blocks // 2):
        last = blocks - 1 - first
        packed.append(
            jnp.concatenate(
                [
                    square[row * LANES : (row + 1) * LANES, row * LANES :]
                    for row in (first, last)
                ],
                axis=1,
            )
        )
    return jnp.concatenate(packed, axis=0)


def unpack_symmetric(packed, size):
    blocks = size // LANES
    rows = [None] * blocks
    for first in range(blocks // 2):
        last = blocks - 1 - first
        both = packed[first * LANES : (first + 1) * LANES]
        cut = size - first * LANES
        rows[first] = jnp.pad(both[:, :cut], ((0, 0), (first * LANES, 0)))
        rows[last] = jnp.pad(both[:, cut:], ((0, 0), (last * LANES, 0)))
    upper = jnp.concatenate(rows, axis=0)
    row_block = lax.broadcasted_iota(jnp.int32, (size, size), 0) // LANES
    col_block = lax.broadcasted_iota(jnp.int32, (size, size), 1) // LANES
    return jnp.where(row_block <= col_block, upper, upper.T)


def mult(left, right):
    return jnp.dot(left, right, precision=PRECISE)


def gramian(rows):
    return jnp.einsum("ri,rj->ij", rows, rows, precision=PRECISE)


def orthogonal_rows(rows, gram):
    factor = 1.0 / (jnp.sqrt(jnp.trace(gram)) + 1e-07)
    rows = rows * factor
    gram = gram * (factor * factor)
    for sweep in range(SWEEPS):
        poly = QUINTIC_B * gram + QUINTIC_C * mult(gram, gram)
        rows = QUINTIC_A * rows + mult(rows, poly)
        if sweep < SWEEPS - 1:
            half = QUINTIC_A * gram + mult(poly, gram)
            gram = QUINTIC_A * half + mult(half, poly)
    return rows


def on_device(
    block_input,
    cotangent,
    gate_proj,
    value_proj,
    bc_proj,
    step_proj,
    out_proj,
    in_gain,
    conv_value,
    conv_bc,
    head_params,
    out_gain,
    m_gate,
    m_value,
    m_bc,
    m_step,
    m_out,
    m_ingain,
    m_convvalue,
    m_convbc,
    m_head,
    m_outgain,
):
    head_count = lax.axis_size("head")
    head_index = lax.axis_index("head")
    seq_count, tokens, _ = block_input.shape
    row_count = gate_proj.shape[0]
    inner_width = gate_proj.shape[1]
    local_heads = step_proj.shape[1]
    bc_width = 2 * STATE // head_count
    model_part = D // head_count
    side_width = -(-(bc_width + local_heads) // LANES) * LANES
    bc_cols_mine = lax.dynamic_slice_in_dim(bc_proj, head_index * bc_width, bc_width, 1)
    side_mine = jnp.concatenate(
        [
            value_proj,
            bc_cols_mine,
            step_proj,
            jnp.zeros((row_count, side_width - bc_width - local_heads), jnp.float32),
        ],
        axis=1,
    )
    mixed_full = lax.all_gather(side_mine, "seq", axis=0, tiled=True)
    gate_full = lax.all_gather(gate_proj, "seq", axis=0, tiled=True)
    out_full = lax.all_gather(out_proj.T, "seq", axis=0, tiled=True)
    conv_mine = lax.dynamic_slice_in_dim(conv_value, head_index * inner_width, inner_width, 1)
    gain_mine = lax.dynamic_slice_in_dim(out_gain, head_index * inner_width, inner_width, 0)
    head_mine = lax.dynamic_slice_in_dim(head_params, head_index * local_heads, local_heads, 1)
    bc_taps = lax.dynamic_slice_in_dim(conv_bc, head_index * bc_width, bc_width, 1)
    inv_rms = lax.rsqrt(jnp.mean(block_input * block_input, axis=-1, keepdims=True) + EPSILON)
    normed = block_input * inv_rms * in_gain
    all_pre = project(normed, mixed_full)
    mixed_width = inner_width + bc_width
    mixed_pre = all_pre[..., :mixed_width]
    step_pre = all_pre[..., mixed_width : mixed_width + local_heads]
    gate_pre = project(normed, gate_full)
    conv_taps = jnp.concatenate([conv_mine, bc_taps], axis=-1)
    edge_rows = from_behind(mixed_pre[:, tokens - (CONV - 1) :, :], "seq", 1)
    padded = jnp.concatenate([edge_rows, mixed_pre], axis=1)
    conv_out = conv_taps[CONV] + sum(
        (conv_taps[offset] * padded[:, offset : offset + tokens, :] for offset in range(CONV))
    )
    activated = jax.nn.silu(conv_out)
    values = activated[..., :inner_width]
    bc_all = lax.all_gather(activated[..., inner_width:], "head", axis=2, tiled=True)
    b_state = bc_all[..., :STATE]
    c_state = bc_all[..., STATE:]
    decay_rate = jnp.exp(head_mine[0])
    skip_gain = head_mine[1]
    step_arg = step_pre + head_mine[2]
    step_size = jax.nn.softplus(step_arg)
    log_decay = -decay_rate * step_size
    base_out, _, summary = group_core(values, step_size, log_decay, b_state, c_state, skip_gain)
    states, totals = gather_states(summary[0], jnp.sum(log_decay, axis=(0, 1)), "seq")
    entry_state = carried_states(states, totals, "seq", False)[None]
    mixer_out = base_out + entry_term(entry_state, log_decay, c_state)
    gate_act = jax.nn.silu(gate_pre)
    gated = mixer_out * gate_act
    square_part = jnp.sum(gated * gated, axis=-1, keepdims=True)
    out_part = back_project(gated * gain_mine, out_full)
    out_sum = lax.psum_scatter(out_part, "head", scatter_dimension=2, tiled=True)
    square_sum = lax.psum(square_part, "head")
    gate_rms = lax.rsqrt(square_sum / DI + EPSILON)
    input_mine = lax.dynamic_slice_in_dim(block_input, head_index * model_part, model_part, 2)
    cotangent_mine = lax.dynamic_slice_in_dim(cotangent, head_index * model_part, model_part, 2)
    block_output = input_mine + gate_rms * out_sum
    normed_out = gated * gate_rms * gain_mine
    grad_outfull = weight_grad(cotangent, normed_out)
    grad_normout = project(cotangent, out_full)
    grad_outgain_mine = jnp.sum(grad_normout * gated * gate_rms, axis=(0, 1))
    scaled = grad_normout * gain_mine
    dot_total = lax.psum(jnp.sum(scaled * gated, axis=-1, keepdims=True), "head")
    grad_gated = gate_rms * scaled - gate_rms**3 * gated * dot_total / DI
    grad_mixer = grad_gated * gate_act
    grad_gate_pre = grad_gated * mixer_out * silu_grad(gate_pre)
    grad_gatefull = weight_grad(normed, grad_gate_pre)
    _, entry_back = jax.vjp(lambda entering: entry_term(entering, log_decay, c_state), entry_state)
    direct = entry_back(grad_mixer)[0]
    directs, _ = gather_states(direct[0], None, "seq")
    leave_grad = carried_states(directs, totals, "seq", True)[None]
    _, mixer_back = jax.vjp(
        full_mixer, values, step_size, log_decay, b_state, c_state, skip_gain, entry_state
    )
    grad_values, grad_stepsize, grad_logdecay, grad_b, grad_c, grad_skip, _ = mixer_back(
        (grad_mixer, leave_grad)
    )
    grad_step_total = grad_stepsize - grad_logdecay * decay_rate
    grad_alog = jnp.sum(grad_logdecay * log_decay, axis=(0, 1))
    grad_step_pre = grad_step_total * jax.nn.sigmoid(step_arg)
    grad_bias = jnp.sum(grad_step_pre, axis=(0, 1))
    grad_bc_all = jnp.concatenate([grad_b, grad_c], axis=-1)
    grad_bc_act = lax.psum_scatter(grad_bc_all, "head", scatter_dimension=2, tiled=True)
    grad_conv = jnp.concatenate([grad_values, grad_bc_act], axis=-1) * silu_grad(conv_out)
    grad_taps = jnp.stack(
        [
            jnp.sum(grad_conv * padded[:, offset : offset + tokens, :], axis=(0, 1))
            for offset in range(CONV)
        ]
        + [jnp.sum(grad_conv, axis=(0, 1))]
    )
    grad_padded = sum(
        (
            jnp.pad(conv_taps[offset] * grad_conv, ((0, 0), (offset, CONV - 1 - offset), (0, 0)))
            for offset in range(CONV)
        )
    )
    edge_back = from_behind(grad_padded[:, : CONV - 1, :], "seq", -1)
    grad_mixed = grad_padded[:, CONV - 1 :, :] + jnp.pad(
        edge_back, ((0, 0), (tokens - (CONV - 1), 0), (0, 0))
    )
    grad_all_pre = jnp.concatenate(
        [
            grad_mixed,
            grad_step_pre,
            jnp.zeros((seq_count, tokens, side_width - bc_width - local_heads), jnp.float32),
        ],
        axis=-1,
    )
    grad_mixedfull = weight_grad(normed, grad_all_pre)
    grad_normed = back_project(grad_gate_pre, gate_full) + back_project(grad_all_pre, mixed_full)
    stat_part = jnp.sum(grad_normed * in_gain * block_input, axis=-1, keepdims=True)
    normed_grad_mine = lax.psum_scatter(grad_normed, "head", scatter_dimension=2, tiled=True)
    stat_total = lax.psum(stat_part, "head")
    gain_part = lax.dynamic_slice_in_dim(in_gain, head_index * model_part, model_part, 0)
    input_grad = (
        cotangent_mine
        + inv_rms * gain_part * normed_grad_mine
        - inv_rms**3 * input_mine * stat_total / D
    )
    grad_ingain_mine = jnp.sum(normed_grad_mine * input_mine * inv_rms, axis=(0, 1))
    grad_out_rows = lax.psum_scatter(grad_outfull, "seq", scatter_dimension=0, tiled=True)
    grad_gate = lax.psum_scatter(grad_gatefull, "seq", scatter_dimension=0, tiled=True)
    grad_mixed_rows = lax.psum_scatter(grad_mixedfull, "seq", scatter_dimension=0, tiled=True)
    grad_value = grad_mixed_rows[:, :inner_width]
    grad_bc = lax.all_gather(
        grad_mixed_rows[:, inner_width:mixed_width], "head", axis=1, tiled=True
    )
    grad_step = grad_mixed_rows[:, mixed_width : mixed_width + local_heads]
    grad_out = grad_out_rows.T
    next_out_rows = MOMENTUM_KEEP * m_out.T + grad_out_rows
    next_gate = MOMENTUM_KEEP * m_gate + grad_gate
    next_value = MOMENTUM_KEEP * m_value + grad_value
    next_bc = MOMENTUM_KEEP * m_bc + grad_bc
    next_step = MOMENTUM_KEEP * m_step + grad_step
    next_out = MOMENTUM_KEEP * m_out + grad_out
    pieces = (
        grad_ingain_mine,
        grad_taps.reshape(-1),
        grad_alog,
        grad_skip,
        grad_bias,
        grad_outgain_mine,
    )
    flat = jnp.concatenate(pieces)
    flat_rows = -(-flat.shape[0] // (8 * LANES)) * 8
    flat = jnp.pad(flat, (0, flat_rows * LANES - flat.shape[0])).reshape(flat_rows, LANES)
    side = 2 * STATE
    small_gram = jnp.pad(gramian(next_step), ((0, -local_heads % 8), (0, side - local_heads)))
    out_gram = lax.psum(pack_symmetric(gramian(next_out_rows)), "seq")
    gate_gram = lax.psum(pack_symmetric(gramian(next_gate)), "seq")
    value_gram, side_gram, flat = lax.psum(
        (
            pack_symmetric(gramian(next_value)),
            jnp.concatenate([gramian(next_bc), small_gram], axis=0),
            flat,
        ),
        "seq",
    )
    flat = lax.all_gather(flat, "head").reshape(head_count, flat_rows * LANES)
    parts = []
    start = 0
    for piece in pieces:
        parts.append(flat[:, start : start + piece.shape[0]])
        start += piece.shape[0]
    grad_ingain = parts[0].reshape(D)
    taps_all = parts[1].reshape(head_count, CONV + 1, mixed_width)
    grad_convvalue = taps_all[:, :, :inner_width].transpose(1, 0, 2).reshape(CONV + 1, DI)
    grad_convbc = taps_all[:, :, inner_width:].transpose(1, 0, 2).reshape(CONV + 1, 2 * STATE)
    grad_head = jnp.stack([parts[2].reshape(H), parts[3].reshape(H), parts[4].reshape(H)])
    grad_outgain = parts[5].reshape(DI)
    next_ingain = MOMENTUM_KEEP * m_ingain + grad_ingain
    next_convvalue = MOMENTUM_KEEP * m_convvalue + grad_convvalue
    next_convbc = MOMENTUM_KEEP * m_convbc + grad_convbc
    next_head = MOMENTUM_KEEP * m_head + grad_head
    next_outgain = MOMENTUM_KEEP * m_outgain + grad_outgain
    update_out = orthogonal_rows(next_out_rows, unpack_symmetric(out_gram, inner_width)).T
    update_gate = orthogonal_rows(next_gate, unpack_symmetric(gate_gram, inner_width))
    update_value = orthogonal_rows(next_value, unpack_symmetric(value_gram, inner_width))
    update_bc = orthogonal_rows(next_bc, side_gram[:side])
    update_step = orthogonal_rows(next_step, side_gram[side : side + local_heads, :local_heads])
    update_scale = MATRIX_RATE * MUON_SCALE * math.sqrt(D)
    new_gate = gate_proj - update_scale * update_gate
    new_value = value_proj - update_scale * update_value
    new_bc = bc_proj - update_scale * update_bc
    new_step = step_proj - update_scale * update_step
    new_out = out_proj - update_scale * update_out
    new_ingain = in_gain - VECTOR_RATE * next_ingain
    new_convvalue = conv_value - VECTOR_RATE * next_convvalue
    new_convbc = conv_bc - VECTOR_RATE * next_convbc
    new_head = head_params - VECTOR_RATE * next_head
    new_outgain = out_gain - VECTOR_RATE * next_outgain
    return (
        block_output,
        input_grad,
        grad_gate,
        grad_value,
        grad_bc,
        grad_step,
        grad_out,
        grad_ingain,
        grad_convvalue,
        grad_convbc,
        grad_head,
        grad_outgain,
        new_gate,
        new_value,
        new_bc,
        new_step,
        new_out,
        new_ingain,
        new_convvalue,
        new_convbc,
        new_head,
        new_outgain,
        next_gate,
        next_value,
        next_bc,
        next_step,
        next_out,
        next_ingain,
        next_convvalue,
        next_convbc,
        next_head,
        next_outgain,
    )


def solution(mesh):
    in_specs = (
        P(None, "seq", None),
        P(None, "seq", None),
        P("seq", "head"),
        P("seq", "head"),
        P("seq", None),
        P("seq", "head"),
        P("head", "seq"),
        P(),
        P(),
        P(),
        P(),
        P(),
        P("seq", "head"),
        P("seq", "head"),
        P("seq", None),
        P("seq", "head"),
        P("head", "seq"),
        P(),
        P(),
        P(),
        P(),
        P(),
    )
    out_specs = (
        P(None, "seq", "head"),
        P(None, "seq", "head"),
        P("seq", "head"),
        P("seq", "head"),
        P("seq", None),
        P("seq", "head"),
        P("head", "seq"),
        P(),
        P(),
        P(),
        P(),
        P(),
        P("seq", "head"),
        P("seq", "head"),
        P("seq", None),
        P("seq", "head"),
        P("head", "seq"),
        P(),
        P(),
        P(),
        P(),
        P(),
        P("seq", "head"),
        P("seq", "head"),
        P("seq", None),
        P("seq", "head"),
        P("head", "seq"),
        P(),
        P(),
        P(),
        P(),
        P(),
    )
    return jax.shard_map(
        on_device, mesh=mesh, in_specs=in_specs, out_specs=out_specs, check_vma=False
    )
```

```python
import functools
import math

import jax
import jax.numpy as jnp
from jax import lax
from jax.experimental import pallas as pl
from jax.experimental.pallas import tpu as pltpu
from jax.sharding import PartitionSpec as P

D = 1536
DI = 3072
STATE = 128
H = 48
GROUP = 256
CONV = 4
SWEEPS = 5


PRECISE = lax.Precision.HIGH
EPSILON = 1e-05
QUINTIC_A = 3.4445
QUINTIC_B = -4.775
QUINTIC_C = 2.0315
MOMENTUM_KEEP = 0.9
MATRIX_RATE = 0.02
VECTOR_RATE = 0.002
MUON_SCALE = 0.2


LANES = 128


def from_behind(value, axis, steps):
    count = lax.axis_size(axis)
    initial, last = (max(0, -steps), min(count, count - steps))
    return lax.ppermute(value, axis, [(source, source + steps) for source in range(initial, last)])


def ring_place(index, count):
    odd = index % 2
    return (1 - odd) * (index // 2) + odd * (count - 1 - index // 2)


def ring_index(position, count):
    position = (position + 2 * count) % count
    back = position // (count // 2)
    return (1 - back) * (2 * position) + back * (2 * (count - 1 - position) + 1)


def greet(axis, neighbours):
    barrier = pltpu.get_barrier_semaphore()
    for neighbour in neighbours:
        pl.semaphore_signal(
            barrier, inc=1, device_id={axis: neighbour}, device_id_type=pl.DeviceIdType.MESH
        )
    pl.semaphore_wait(barrier, len(neighbours))


def piece_count(half, arrays):
    return 2 if arrays == 1 and half % 16 == 0 else 1


def relay_step(axis, count, backward, refs):
    own, decay, near, entering, leaving, send_sem, recv_sem = refs
    me = lax.axis_index(axis)
    order = count - 1 - me if backward else me
    ahead = (me + count - 1) % count if backward else (me + 1) % count
    copy = pltpu.make_async_remote_copy(
        src_ref=leaving,
        dst_ref=entering,
        send_sem=send_sem,
        recv_sem=recv_sem,
        device_id={axis: ahead},
        device_id_type=pl.DeviceIdType.MESH,
    )

    def turn(at):
        @pl.when(order == at)
        def _():
            if at:
                copy.wait_recv()
                near[...] = entering[...]
                if at < count - 1:
                    leaving[...] = own[...] + decay[...] * entering[...]
            else:
                near[...] = jnp.zeros_like(near)
                leaving[...] = own[...]
            if at < count - 1:
                copy.start()

    def finish():
        turn(count - 1)

        @pl.when(order < count - 1)
        def _():
            copy.wait_send()

    return turn, finish


def relay_parts(relay):
    if relay is None:
        return [], [], []
    state = relay[0]
    buffers = [pltpu.VMEM(state.shape, state.dtype)] * 2
    return (
        [relay[0], relay[1]],
        [jax.ShapeDtypeStruct(state.shape, state.dtype)],
        buffers + [pltpu.SemaphoreType.DMA(()), pltpu.SemaphoreType.DMA(())],
    )


def ring_neighbours(axis, count, relayed):
    me = lax.axis_index(axis)
    place = ring_place(me, count)
    right, left = ring_index(place + 1, count), ring_index(place - 1, count)
    greeted = (left, right)
    if relayed:
        greeted += ((me + 1) % count, (me + count - 1) % count)
    greet(axis, greeted)
    return me, place, right, left


def ring_gather_kernel(axis, count, arrays, backward, *refs):
    relayed = backward is not None
    turn, finish = (lambda at: None), (lambda: None)
    if relayed:
        states, refs = refs[:2], refs[2:]
        near, refs = refs[2 * arrays], refs[: 2 * arrays] + refs[2 * arrays + 1 :]
        turn, finish = relay_step(axis, count, backward, (*states, near, *refs[-4:]))
        refs = refs[:-4]
    shards, outs = refs[:arrays], refs[arrays : 2 * arrays]
    send_sem, recv_sem, own_sem = refs[2 * arrays :]
    me, place, right, left = ring_neighbours(axis, count, relayed)
    own = []
    for j in range(arrays):
        rows = shards[j].shape[0]
        start = pl.multiple_of(me * rows, 8)
        own.append(
            pltpu.make_async_copy(shards[j], outs[j].at[pl.ds(start, rows)], own_sem.at[j])
        )
    flights = {}
    for step in range(count - 1):
        for j in range(arrays):
            rows = shards[j].shape[0]
            pieces = piece_count(rows // 2, arrays)
            length = rows // 2 // pieces
            for piece in range(pieces):
                for way, sign, target in ((0, -1, right), (1, 1, left)):
                    origin = ring_index(place + sign * step, count)
                    within = (way * pieces + piece) * length
                    region = pl.ds(pl.multiple_of(origin * rows + within, 8), length)
                    if step:
                        flights[step - 1, j, piece, way].wait_recv()
                        source = outs[j].at[region]
                    else:
                        source = shards[j].at[pl.ds(within, length)]
                    flight = pltpu.make_async_remote_copy(
                        src_ref=source,
                        dst_ref=outs[j].at[region],
                        send_sem=send_sem.at[way, j + piece, step],
                        recv_sem=recv_sem.at[way, j + piece, step],
                        device_id={axis: target},
                        device_id_type=pl.DeviceIdType.MESH,
                    )
                    flights[step, j, piece, way] = flight
                    flight.start()
        if step == 0:
            for copy in own:
                copy.start()
        turn(step)
    for (step, *_), flight in flights.items():
        if step == count - 2:
            flight.wait_recv()
    finish()
    for copy in own:
        copy.wait()
    for flight in flights.values():
        flight.wait_send()


def busy_cost(sent):
    return pl.CostEstimate(flops=6000 * sent, bytes_accessed=2 * sent, transcendentals=0)


def ring_gather(shards, axis, collective_id, relay=None):
    count = lax.axis_size(axis)
    arrays = len(shards)
    states, near, relay_scratch = relay_parts(relay)
    backward = None if relay is None else relay[2]
    sent = sum(shard.size for shard in shards) * 4 * (count - 1)
    return pl.pallas_call(
        functools.partial(ring_gather_kernel, axis, count, arrays, backward),
        out_shape=[
            jax.ShapeDtypeStruct((count * shard.shape[0], shard.shape[1]), shard.dtype)
            for shard in shards
        ]
        + near,
        in_specs=[pl.BlockSpec(memory_space=pltpu.VMEM)] * (arrays + len(states)),
        out_specs=[pl.BlockSpec(memory_space=pl.ANY)] * arrays
        + [pl.BlockSpec(memory_space=pltpu.VMEM)] * len(near),
        scratch_shapes=[
            pltpu.SemaphoreType.DMA((2, max(arrays, 2), count - 1)),
            pltpu.SemaphoreType.DMA((2, max(arrays, 2), count - 1)),
            pltpu.SemaphoreType.DMA((arrays,)),
        ]
        + relay_scratch,
        compiler_params=pltpu.CompilerParams(collective_id=collective_id, has_side_effects=True),
        cost_estimate=busy_cost(sent),
        name=f"ring_gather_{collective_id}",
    )(*states, *shards)


def ring_scatter_kernel(axis, count, arrays, backward, *refs):
    relayed = backward is not None
    turn, finish = (lambda at: None), (lambda: None)
    if relayed:
        states, refs = refs[:2], refs[2:]
        near, refs = refs[2 * arrays], refs[: 2 * arrays] + refs[2 * arrays + 1 :]
        turn, finish = relay_step(axis, count, backward, (*states, near, *refs[-4:]))
        refs = refs[:-4]
    parts, outs, slots = refs[:arrays], refs[arrays : 2 * arrays], refs[2 * arrays : 3 * arrays]
    send_sem, recv_sem = refs[3 * arrays :]
    me, place, right, left = ring_neighbours(axis, count, relayed)
    flights = {}
    for step in range(count):
        for j in range(arrays):
            rows = outs[j].shape[0]
            pieces = piece_count(rows // 2, arrays)
            length = rows // 2 // pieces
            for piece in range(pieces):
                part = pl.ds(piece * length, length)
                for way, sign, target in ((0, -1, right), (1, 1, left)):
                    goal = ring_index(place + sign * (1 + step), count)
                    within = (way * pieces + piece) * length
                    region = pl.ds(pl.multiple_of(goal * rows + within, 8), length)
                    if step:
                        flights[step - 1, j, piece, way].wait_recv()
                        total = slots[j][way, step - 1, part, :] + parts[j][region, :]
                        if step == count - 1:
                            outs[j][pl.ds(within, length), :] = total
                            continue
                        slots[j][way, step - 1, part, :] = total
                        source = slots[j].at[way, step - 1, part]
                    else:
                        source = parts[j].at[region]
                    flight = pltpu.make_async_remote_copy(
                        src_ref=source,
                        dst_ref=slots[j].at[way, step, part],
                        send_sem=send_sem.at[way, j + piece, step],
                        recv_sem=recv_sem.at[way, j + piece, step],
                        device_id={axis: target},
                        device_id_type=pl.DeviceIdType.MESH,
                    )
                    flights[step, j, piece, way] = flight
                    flight.start()
        if step < count - 1:
            turn(step)
    finish()
    for flight in flights.values():
        flight.wait_send()


def ring_scatter(parts, axis, collective_id, relay=None):
    count = lax.axis_size(axis)
    arrays = len(parts)
    states, near, relay_scratch = relay_parts(relay)
    backward = None if relay is None else relay[2]
    shapes = [(part.shape[0] // count, part.shape[1]) for part in parts]
    sent = sum(part.size for part in parts) * 4
    return pl.pallas_call(
        functools.partial(ring_scatter_kernel, axis, count, arrays, backward),
        out_shape=[jax.ShapeDtypeStruct(shape, jnp.float32) for shape in shapes] + near,
        in_specs=[pl.BlockSpec(memory_space=pltpu.VMEM)] * (arrays + len(states)),
        out_specs=[pl.BlockSpec(memory_space=pltpu.VMEM)] * (arrays + len(near)),
        scratch_shapes=[
            pltpu.VMEM((2, count - 1, rows // 2, columns), jnp.float32) for rows, columns in shapes
        ]
        + [
            pltpu.SemaphoreType.DMA((2, max(arrays, 2), count - 1)),
            pltpu.SemaphoreType.DMA((2, max(arrays, 2), count - 1)),
        ]
        + relay_scratch,
        compiler_params=pltpu.CompilerParams(collective_id=collective_id, has_side_effects=True),
        cost_estimate=busy_cost(sent),
        name=f"ring_scatter_{collective_id}",
    )(*states, *parts)


def silu_grad(pre_value):
    sigmoid_val = jax.nn.sigmoid(pre_value)
    return sigmoid_val * (1.0 + pre_value * (1.0 - sigmoid_val))


def project(activation, weight):
    return jnp.einsum("std,dk->stk", activation, weight, precision=PRECISE)


def back_project(upstream, weight):
    return jnp.einsum("stk,dk->std", upstream, weight, precision=PRECISE)


def weight_grad(activation, upstream):
    return jnp.einsum("std,stk->dk", activation, upstream, precision=PRECISE)


def place_slice(portion, full_size, offset, along):
    full_shape = list(portion.shape)
    full_shape[along] = full_size
    return lax.dynamic_update_slice_in_dim(
        jnp.zeros(full_shape, jnp.float32), portion, offset, along
    )


def running_decay(log_decay):
    seq_count, tokens, head_count = log_decay.shape
    blocks = tokens // GROUP
    grouped = log_decay.reshape(seq_count, blocks, GROUP, head_count)
    rows_at = lax.broadcasted_iota(jnp.int32, (GROUP, GROUP), 0)
    cols_at = lax.broadcasted_iota(jnp.int32, (GROUP, GROUP), 1)
    lower_mask = rows_at >= cols_at
    within = jnp.einsum("ij,sbjh->sbih", lower_mask.astype(jnp.float32), grouped, precision=PRECISE)
    group_total = within[:, :, -1, :]
    through = jnp.cumsum(group_total, axis=1)
    before = through - group_total
    return (lower_mask, within, group_total, through, before)


def group_core(values, step_size, log_decay, b_state, c_state, skip_gain):
    seq_count, tokens, width = values.shape
    head_count = step_size.shape[2]
    head_dim = width // head_count
    blocks = tokens // GROUP
    lower_mask, within, group_total, through, before = running_decay(log_decay)
    head_values = values.reshape(seq_count, blocks, GROUP, head_count, head_dim)
    step_blocks = step_size.reshape(seq_count, blocks, GROUP, head_count)
    b_blocks = b_state.reshape(seq_count, blocks, GROUP, -1)
    c_blocks = c_state.reshape(seq_count, blocks, GROUP, -1)
    decay_rows = within.transpose(0, 1, 3, 2)
    log_gaps = decay_rows[..., :, None] - decay_rows[..., None, :]
    decay_mat = jnp.where(lower_mask, jnp.exp(jnp.where(lower_mask, log_gaps, 0.0)), 0.0)
    scores = jnp.einsum("sbin,sbjn->sbij", c_blocks, b_blocks, precision=PRECISE)
    weighted = scores[:, :, None] * decay_mat * step_blocks.transpose(0, 1, 3, 2)[:, :, :, None, :]
    intra_out = jnp.einsum("sbhij,sbjhp->sbihp", weighted, head_values, precision=PRECISE)
    to_end = jnp.exp(group_total[:, :, None, :] - within) * step_blocks
    states = jnp.einsum("sbjh,sbjhp,sbjn->sbhpn", to_end, head_values, b_blocks, precision=PRECISE)
    later_at = lax.broadcasted_iota(jnp.int32, (blocks, blocks), 0)
    earlier_at = lax.broadcasted_iota(jnp.int32, (blocks, blocks), 1)
    earlier_mask = (later_at > earlier_at)[None, :, :, None]
    carry_gap = before[:, :, None, :] - through[:, None, :, :]
    carry_factor = jnp.where(earlier_mask, jnp.exp(jnp.where(earlier_mask, carry_gap, 0.0)), 0.0)
    entering = jnp.einsum("skmh,smhpn->skhpn", carry_factor, states, precision=PRECISE)
    inter_out = (
        jnp.einsum("sbin,sbhpn->sbihp", c_blocks, entering, precision=PRECISE)
        * jnp.exp(within)[..., None]
    )
    output = intra_out + inter_out + skip_gain[:, None] * head_values
    end_gap = through - through
    summary = jnp.einsum("sbh,sbhpn->shpn", jnp.exp(end_gap), states, precision=PRECISE)
    decay_all = jnp.exp(through[:, -1, :])
    return (output.reshape(seq_count, tokens, width), decay_all, summary)


def entry_term(entry_state, log_decay, c_state):
    seq_count, tokens, head_count = log_decay.shape
    blocks = tokens // GROUP
    _, within, _, _, before = running_decay(log_decay)
    reach = jnp.exp(within + before[:, :, None, :])
    c_blocks = c_state.reshape(seq_count, blocks, GROUP, -1)
    result = (
        jnp.einsum("sbin,shpn->sbihp", c_blocks, entry_state, precision=PRECISE) * reach[..., None]
    )
    return result.reshape(seq_count, tokens, -1)


def full_mixer(values, step_size, log_decay, b_state, c_state, skip_gain, entry_state):
    base_out, decay_all, summary = group_core(
        values, step_size, log_decay, b_state, c_state, skip_gain
    )
    output = base_out + entry_term(entry_state, log_decay, c_state)
    leaving = decay_all[..., None, None] * entry_state + summary
    return (output, leaving)


def halves(value):
    high = value.astype(jnp.bfloat16)
    return high, (value - high.astype(jnp.float32)).astype(jnp.bfloat16)


def three_pass(left, right):
    def one(a, b):
        return jnp.dot(a, b, preferred_element_type=jnp.float32)

    return one(left[0], right[0]) + (one(left[0], right[1]) + one(left[1], right[0]))


def gram_strips(rows):
    size = rows.shape[1]
    block = min(size, 256)
    return [
        jnp.einsum("ri,rj->ij", rows[:, at : at + block], rows[:, at:], precision=PRECISE)
        for at in range(0, size, block)
    ]


def orthogonal_kernel(arrays, strip_counts, *refs):

    grams = []
    for strips in strip_counts:
        grams.append(refs[:strips])
        refs = refs[strips:]
    rows, outs, scratch = refs[:arrays], refs[arrays : 2 * arrays], refs[2 * arrays :]
    work = [scratch[8 * j : 8 * j + 8] for j in range(arrays)]
    for j in range(arrays):
        whole = work[j][0]
        block = grams[j][0].shape[0]
        spots = [slice(at * block, (at + 1) * block) for at in range(len(grams[j]))]
        across = lax.broadcasted_iota(jnp.int32, (block, block), 0)
        down = lax.broadcasted_iota(jnp.int32, (block, block), 1)
        total = jnp.zeros((1, 1), jnp.float32)
        for strip in grams[j]:
            diagonal = jnp.where(across == down, strip[:, :block], 0.0)
            total += jnp.sum(jnp.sum(diagonal, axis=0, keepdims=True), axis=1, keepdims=True)
        factor = 1.0 / (jnp.sqrt(total) + 1e-07)
        square = factor * factor
        for i, strip in enumerate(grams[j]):
            for k in range(i, len(spots)):
                piece = strip[:, (k - i) * block : (k - i + 1) * block] * square
                whole[spots[i], spots[k]] = piece
                if i != k:
                    whole[spots[k], spots[i]] = piece.T
        outs[j][...] = rows[j][...] * factor

    def split_whole(j, at):
        whole, high, low = work[j][0], work[j][1], work[j][2]
        high[at, :], low[at, :] = halves(whole[at, :])

    def sweep(last):
        strips = []
        for j in range(arrays):
            size = rows[j].shape[1]
            strip = min(size, 256)
            strips.append([slice(s, s + strip) for s in range(0, size, strip)])
        for j in range(arrays):
            for at in strips[j]:
                split_whole(j, at)
        for j in range(arrays):
            whole, high, low, poly_h, poly_l, _, _, _ = work[j]
            for at in strips[j]:
                poly = QUINTIC_B * whole[at, :] + QUINTIC_C * three_pass(
                    (high[at, :], low[at, :]), (high[...], low[...])
                )
                poly_h[at, :], poly_l[at, :] = halves(poly)
        for j in range(arrays):
            poly = (work[j][3][...], work[j][4][...])
            value = outs[j][...]
            outs[j][...] = QUINTIC_A * value + three_pass(halves(value), poly)
        if last:
            return
        for j in range(arrays):
            whole, high, low, poly_h, poly_l, half, half_h, half_l = work[j]
            for at in strips[j]:
                value = QUINTIC_A * whole[at, :] + three_pass(
                    (poly_h[at, :], poly_l[at, :]), (high[...], low[...])
                )
                half[at, :] = value
                half_h[at, :], half_l[at, :] = halves(value)
        for j in range(arrays):
            whole, _, _, poly_h, poly_l, half, half_h, half_l = work[j]
            for at in strips[j]:
                whole[at, :] = QUINTIC_A * half[at, :] + three_pass(
                    (half_h[at, :], half_l[at, :]), (poly_h[...], poly_l[...])
                )

    def body(_, carry):
        sweep(False)
        return carry

    lax.fori_loop(0, SWEEPS - 1, body, 0)
    sweep(True)


def orthogonal_rows(pairs, name):
    arrays = len(pairs)
    scratch = []
    flops = 0
    for _, rows in pairs:
        size = rows.shape[1]
        full, narrow = pltpu.VMEM((size, size), jnp.float32), pltpu.VMEM((size, size), jnp.bfloat16)
        scratch += [full, narrow, narrow, narrow, narrow, full, narrow, narrow]
        flops += 6 * (13 * size**3 + 5 * rows.shape[0] * size**2)
    return pl.pallas_call(
        functools.partial(orthogonal_kernel, arrays, [len(strips) for strips, _ in pairs]),
        out_shape=[jax.ShapeDtypeStruct(rows.shape, jnp.float32) for _, rows in pairs],
        in_specs=[pl.BlockSpec(memory_space=pltpu.VMEM)]
        * (arrays + sum(len(strips) for strips, _ in pairs)),
        out_specs=[pl.BlockSpec(memory_space=pltpu.VMEM)] * arrays,
        scratch_shapes=scratch,
        cost_estimate=pl.CostEstimate(flops=flops, bytes_accessed=0, transcendentals=0),
        name=name,
    )(*[strip for strips, _ in pairs for strip in strips], *[rows for _, rows in pairs])


def on_device(
    block_input,
    cotangent,
    gate_proj,
    value_proj,
    bc_proj,
    step_proj,
    out_proj,
    in_gain,
    conv_value,
    conv_bc,
    head_params,
    out_gain,
    m_gate,
    m_value,
    m_bc,
    m_step,
    m_out,
    m_ingain,
    m_convvalue,
    m_convbc,
    m_head,
    m_outgain,
):
    head_count = lax.axis_size("head")
    head_index = lax.axis_index("head")
    seq_count, tokens, _ = block_input.shape
    row_count = gate_proj.shape[0]
    inner_width = gate_proj.shape[1]
    local_heads = step_proj.shape[1]
    bc_width = 2 * STATE // head_count
    model_part = D // head_count
    side_width = -(-(bc_width + local_heads) // LANES) * LANES
    bc_cols_mine = lax.dynamic_slice_in_dim(bc_proj, head_index * bc_width, bc_width, 1)
    side_mine = jnp.concatenate(
        [
            value_proj,
            bc_cols_mine,
            step_proj,
            jnp.zeros((row_count, side_width - bc_width - local_heads), jnp.float32),
        ],
        axis=1,
    )
    (mixed_full,) = ring_gather((side_mine,), "seq", 0)
    conv_mine = lax.dynamic_slice_in_dim(conv_value, head_index * inner_width, inner_width, 1)
    gain_mine = lax.dynamic_slice_in_dim(out_gain, head_index * inner_width, inner_width, 0)
    head_mine = lax.dynamic_slice_in_dim(head_params, head_index * local_heads, local_heads, 1)
    bc_taps = lax.dynamic_slice_in_dim(conv_bc, head_index * bc_width, bc_width, 1)
    inv_rms = lax.rsqrt(jnp.mean(block_input * block_input, axis=-1, keepdims=True) + EPSILON)
    normed = block_input * inv_rms * in_gain
    all_pre = project(normed, mixed_full)
    mixed_width = inner_width + bc_width
    mixed_pre = all_pre[..., :mixed_width]
    step_pre = all_pre[..., mixed_width : mixed_width + local_heads]
    conv_taps = jnp.concatenate([conv_mine, bc_taps], axis=-1)
    edge_rows = from_behind(mixed_pre[:, tokens - (CONV - 1) :, :], "seq", 1)
    padded = jnp.concatenate([edge_rows, mixed_pre], axis=1)
    conv_out = conv_taps[CONV] + sum(
        (conv_taps[offset] * padded[:, offset : offset + tokens, :] for offset in range(CONV))
    )
    activated = jax.nn.silu(conv_out)
    values = activated[..., :inner_width]
    bc_all = lax.all_gather(activated[..., inner_width:], "head", axis=2, tiled=True)
    b_state = bc_all[..., :STATE]
    c_state = bc_all[..., STATE:]
    decay_rate = jnp.exp(head_mine[0])
    skip_gain = head_mine[1]
    step_arg = step_pre + head_mine[2]
    step_size = jax.nn.softplus(step_arg)
    log_decay = -decay_rate * step_size
    base_out, decay_all, summary = group_core(
        values, step_size, log_decay, b_state, c_state, skip_gain
    )
    state_shape = summary.shape
    state_rows = (-1, state_shape[-1])
    decay_rows = jnp.broadcast_to(decay_all[..., None, None], state_shape).reshape(state_rows)
    gate_full, out_full, entry_rows = ring_gather(
        (gate_proj, out_proj.T), "seq", 1, (summary.reshape(state_rows), decay_rows, False)
    )
    entry_state = entry_rows.reshape(state_shape)
    gate_pre = project(normed, gate_full)
    mixer_out = base_out + entry_term(entry_state, log_decay, c_state)
    gate_act = jax.nn.silu(gate_pre)
    gated = mixer_out * gate_act
    square_part = jnp.sum(gated * gated, axis=-1, keepdims=True)
    out_part = back_project(gated * gain_mine, out_full)
    out_sum = lax.psum_scatter(out_part, "head", scatter_dimension=2, tiled=True)
    square_sum = lax.psum(square_part, "head")
    gate_rms = lax.rsqrt(square_sum / DI + EPSILON)
    input_mine = lax.dynamic_slice_in_dim(block_input, head_index * model_part, model_part, 2)
    cotangent_mine = lax.dynamic_slice_in_dim(cotangent, head_index * model_part, model_part, 2)
    block_output = input_mine + gate_rms * out_sum
    normed_out = gated * gate_rms * gain_mine
    grad_outfull = weight_grad(cotangent, normed_out)
    grad_normout = project(cotangent, out_full)
    grad_outgain_mine = jnp.sum(grad_normout * gated * gate_rms, axis=(0, 1))
    scaled = grad_normout * gain_mine
    dot_total = lax.psum(jnp.sum(scaled * gated, axis=-1, keepdims=True), "head")
    grad_gated = gate_rms * scaled - gate_rms**3 * gated * dot_total / DI
    grad_mixer = grad_gated * gate_act
    grad_gate_pre = grad_gated * mixer_out * silu_grad(gate_pre)
    grad_gatefull = weight_grad(normed, grad_gate_pre)
    _, entry_back = jax.vjp(lambda entering: entry_term(entering, log_decay, c_state), entry_state)
    direct = entry_back(grad_mixer)[0]
    grad_out_rows, grad_gate, leave_rows = ring_scatter(
        (grad_outfull, grad_gatefull), "seq", 2, (direct.reshape(state_rows), decay_rows, True)
    )
    leave_grad = leave_rows.reshape(state_shape)
    _, mixer_back = jax.vjp(
        full_mixer, values, step_size, log_decay, b_state, c_state, skip_gain, entry_state
    )
    grad_values, grad_stepsize, grad_logdecay, grad_b, grad_c, grad_skip, _ = mixer_back(
        (grad_mixer, leave_grad)
    )
    grad_step_total = grad_stepsize - grad_logdecay * decay_rate
    grad_alog = jnp.sum(grad_logdecay * log_decay, axis=(0, 1))
    grad_step_pre = grad_step_total * jax.nn.sigmoid(step_arg)
    grad_bias = jnp.sum(grad_step_pre, axis=(0, 1))
    grad_bc_all = jnp.concatenate([grad_b, grad_c], axis=-1)
    grad_bc_act = lax.psum_scatter(grad_bc_all, "head", scatter_dimension=2, tiled=True)
    grad_conv = jnp.concatenate([grad_values, grad_bc_act], axis=-1) * silu_grad(conv_out)
    grad_taps = jnp.stack(
        [
            jnp.sum(grad_conv * padded[:, offset : offset + tokens, :], axis=(0, 1))
            for offset in range(CONV)
        ]
        + [jnp.sum(grad_conv, axis=(0, 1))]
    )
    grad_padded = sum(
        (
            jnp.pad(conv_taps[offset] * grad_conv, ((0, 0), (offset, CONV - 1 - offset), (0, 0)))
            for offset in range(CONV)
        )
    )
    edge_back = from_behind(grad_padded[:, : CONV - 1, :], "seq", -1)
    grad_mixed = grad_padded[:, CONV - 1 :, :] + jnp.pad(
        edge_back, ((0, 0), (tokens - (CONV - 1), 0), (0, 0))
    )
    grad_all_pre = jnp.concatenate(
        [
            grad_mixed,
            grad_step_pre,
            jnp.zeros((seq_count, tokens, side_width - bc_width - local_heads), jnp.float32),
        ],
        axis=-1,
    )
    grad_mixedfull = weight_grad(normed, grad_all_pre)
    grad_normed = back_project(grad_gate_pre, gate_full) + back_project(grad_all_pre, mixed_full)
    stat_part = jnp.sum(grad_normed * in_gain * block_input, axis=-1, keepdims=True)
    normed_grad_mine = lax.psum_scatter(grad_normed, "head", scatter_dimension=2, tiled=True)
    stat_total = lax.psum(stat_part, "head")
    gain_part = lax.dynamic_slice_in_dim(in_gain, head_index * model_part, model_part, 0)
    input_grad = (
        cotangent_mine
        + inv_rms * gain_part * normed_grad_mine
        - inv_rms**3 * input_mine * stat_total / D
    )
    grad_ingain_part = jnp.sum(grad_normed * block_input * inv_rms, axis=(0, 1))
    (grad_mixed_rows,) = ring_scatter((grad_mixedfull,), "seq", 3)
    grad_value = grad_mixed_rows[:, :inner_width]
    grad_bc = lax.all_gather(
        grad_mixed_rows[:, inner_width:mixed_width], "head", axis=1, tiled=True
    )
    grad_step = grad_mixed_rows[:, mixed_width : mixed_width + local_heads]
    grad_out = grad_out_rows.T
    next_out_rows = MOMENTUM_KEEP * m_out.T + grad_out_rows
    next_gate = MOMENTUM_KEEP * m_gate + grad_gate
    next_value = MOMENTUM_KEEP * m_value + grad_value
    next_bc = MOMENTUM_KEEP * m_bc + grad_bc
    next_step = MOMENTUM_KEEP * m_step + grad_step
    next_out = MOMENTUM_KEEP * m_out + grad_out
    pieces = (
        grad_ingain_part,
        grad_taps.reshape(-1),
        grad_alog,
        grad_skip,
        grad_bias,
        grad_outgain_mine,
    )
    flat = jnp.concatenate(pieces)
    flat_rows = -(-flat.shape[0] // (16 * STATE)) * 8
    flat = jnp.pad(flat, (0, flat_rows * 2 * STATE - flat.shape[0])).reshape(flat_rows, 2 * STATE)
    side = 2 * STATE
    strips = len(gram_strips(next_gate))
    early = lax.psum(gram_strips(next_out_rows) + gram_strips(next_gate), "seq")
    out_gram, gate_gram = early[:strips], early[strips:]
    late_value, _ = lax.optimization_barrier((next_value, early))
    (step_gram,) = gram_strips(next_step)
    step_gram = jnp.pad(step_gram, ((0, -local_heads % 8), (0, side - local_heads)))
    late = lax.psum(
        gram_strips(late_value)
        + [jnp.concatenate(gram_strips(next_bc) + [step_gram, flat], axis=0)],
        "seq",
    )
    value_gram, side_gram = late[:-1], late[-1]
    flat = side_gram[side + step_gram.shape[0] :]
    step_gram = jnp.pad(
        side_gram[side : side + step_gram.shape[0], :LANES],
        ((0, LANES - step_gram.shape[0]), (0, 0)),
    )
    flat = lax.all_gather(flat, "head").reshape(head_count, flat_rows * 2 * STATE)
    parts = []
    start = 0
    for piece in pieces:
        parts.append(flat[:, start : start + piece.shape[0]])
        start += piece.shape[0]
    grad_ingain = jnp.sum(parts[0], axis=0)
    taps_all = parts[1].reshape(head_count, CONV + 1, mixed_width)
    grad_convvalue = taps_all[:, :, :inner_width].transpose(1, 0, 2).reshape(CONV + 1, DI)
    grad_convbc = taps_all[:, :, inner_width:].transpose(1, 0, 2).reshape(CONV + 1, 2 * STATE)
    grad_head = jnp.stack([parts[2].reshape(H), parts[3].reshape(H), parts[4].reshape(H)])
    grad_outgain = parts[5].reshape(DI)
    next_ingain = MOMENTUM_KEEP * m_ingain + grad_ingain
    next_convvalue = MOMENTUM_KEEP * m_convvalue + grad_convvalue
    next_convbc = MOMENTUM_KEEP * m_convbc + grad_convbc
    next_head = MOMENTUM_KEEP * m_head + grad_head
    next_outgain = MOMENTUM_KEEP * m_outgain + grad_outgain
    update_out, update_gate = orthogonal_rows(
        ((out_gram, next_out_rows), (gate_gram, next_gate)), "ortho_first"
    )
    update_out = update_out.T
    update_value, update_bc, update_step = orthogonal_rows(
        (
            (value_gram, next_value),
            ([side_gram[:side]], next_bc),
            ([step_gram], jnp.pad(next_step, ((0, 0), (0, LANES - local_heads)))),
        ),
        "ortho_last",
    )
    update_step = update_step[:, :local_heads]
    update_scale = MATRIX_RATE * MUON_SCALE * math.sqrt(D)
    new_gate = gate_proj - update_scale * update_gate
    new_value = value_proj - update_scale * update_value
    new_bc = bc_proj - update_scale * update_bc
    new_step = step_proj - update_scale * update_step
    new_out = out_proj - update_scale * update_out
    new_ingain = in_gain - VECTOR_RATE * next_ingain
    new_convvalue = conv_value - VECTOR_RATE * next_convvalue
    new_convbc = conv_bc - VECTOR_RATE * next_convbc
    new_head = head_params - VECTOR_RATE * next_head
    new_outgain = out_gain - VECTOR_RATE * next_outgain
    return (
        block_output,
        input_grad,
        grad_gate,
        grad_value,
        grad_bc,
        grad_step,
        grad_out,
        grad_ingain,
        grad_convvalue,
        grad_convbc,
        grad_head,
        grad_outgain,
        new_gate,
        new_value,
        new_bc,
        new_step,
        new_out,
        new_ingain,
        new_convvalue,
        new_convbc,
        new_head,
        new_outgain,
        next_gate,
        next_value,
        next_bc,
        next_step,
        next_out,
        next_ingain,
        next_convvalue,
        next_convbc,
        next_head,
        next_outgain,
    )


def solution(mesh):
    in_specs = (
        P(None, "seq", None),
        P(None, "seq", None),
        P("seq", "head"),
        P("seq", "head"),
        P("seq", None),
        P("seq", "head"),
        P("head", "seq"),
        P(),
        P(),
        P(),
        P(),
        P(),
        P("seq", "head"),
        P("seq", "head"),
        P("seq", None),
        P("seq", "head"),
        P("head", "seq"),
        P(),
        P(),
        P(),
        P(),
        P(),
    )
    out_specs = (
        P(None, "seq", "head"),
        P(None, "seq", "head"),
        P("seq", "head"),
        P("seq", "head"),
        P("seq", None),
        P("seq", "head"),
        P("head", "seq"),
        P(),
        P(),
        P(),
        P(),
        P(),
        P("seq", "head"),
        P("seq", "head"),
        P("seq", None),
        P("seq", "head"),
        P("head", "seq"),
        P(),
        P(),
        P(),
        P(),
        P(),
        P("seq", "head"),
        P("seq", "head"),
        P("seq", None),
        P("seq", "head"),
        P("head", "seq"),
        P(),
        P(),
        P(),
        P(),
        P(),
    )
    return jax.shard_map(
        on_device, mesh=mesh, in_specs=in_specs, out_specs=out_specs, check_vma=False
    )
```

```python
import functools
import math

import jax
import jax.numpy as jnp
from jax import lax
from jax.experimental import pallas as pl
from jax.experimental.pallas import tpu as pltpu
from jax.sharding import PartitionSpec as P

D = 1536
DI = 3072
STATE = 128
H = 48
GROUP = 256
CONV = 4
SWEEPS = 5


PRECISE = lax.Precision.HIGH
EPSILON = 1e-05
QUINTIC_A = 3.4445
QUINTIC_B = -4.775
QUINTIC_C = 2.0315
MOMENTUM_KEEP = 0.9
MATRIX_RATE = 0.02
VECTOR_RATE = 0.002
MUON_SCALE = 0.2


LANES = 128


def from_behind(value, axis, steps):
    count = lax.axis_size(axis)
    initial, last = (max(0, -steps), min(count, count - steps))
    return lax.ppermute(value, axis, [(source, source + steps) for source in range(initial, last)])


def ring_place(index, count):
    odd = index % 2
    return (1 - odd) * (index // 2) + odd * (count - 1 - index // 2)


def ring_index(position, count):
    position = (position + 2 * count) % count
    back = position // (count // 2)
    return (1 - back) * (2 * position) + back * (2 * (count - 1 - position) + 1)


def greet(axis, neighbours):
    barrier = pltpu.get_barrier_semaphore()
    for neighbour in neighbours:
        pl.semaphore_signal(
            barrier, inc=1, device_id={axis: neighbour}, device_id_type=pl.DeviceIdType.MESH
        )
    pl.semaphore_wait(barrier, len(neighbours))


def piece_count(half, arrays):
    return 2 if arrays == 1 and half % 16 == 0 else 1


def relay_step(axis, count, backward, refs):
    own, decay, near, entering, leaving, send_sem, recv_sem = refs
    me = lax.axis_index(axis)
    order = count - 1 - me if backward else me
    ahead = (me + count - 1) % count if backward else (me + 1) % count
    copy = pltpu.make_async_remote_copy(
        src_ref=leaving,
        dst_ref=entering,
        send_sem=send_sem,
        recv_sem=recv_sem,
        device_id={axis: ahead},
        device_id_type=pl.DeviceIdType.MESH,
    )

    def turn(at):
        @pl.when(order == at)
        def _():
            if at:
                copy.wait_recv()
                near[...] = entering[...]
                if at < count - 1:
                    leaving[...] = own[...] + decay[...] * entering[...]
            else:
                near[...] = jnp.zeros_like(near)
                leaving[...] = own[...]
            if at < count - 1:
                copy.start()

    def finish():
        turn(count - 1)

        @pl.when(order < count - 1)
        def _():
            copy.wait_send()

    return turn, finish


def relay_parts(relay):
    if relay is None:
        return [], [], []
    state = relay[0]
    buffers = [pltpu.VMEM(state.shape, state.dtype)] * 2
    return (
        [relay[0], relay[1]],
        [jax.ShapeDtypeStruct(state.shape, state.dtype)],
        buffers + [pltpu.SemaphoreType.DMA(()), pltpu.SemaphoreType.DMA(())],
    )


def ring_neighbours(axis, count, relayed):
    me = lax.axis_index(axis)
    place = ring_place(me, count)
    right, left = ring_index(place + 1, count), ring_index(place - 1, count)
    greeted = (left, right)
    if relayed:
        greeted += ((me + 1) % count, (me + count - 1) % count)
    greet(axis, greeted)
    return me, place, right, left


def halves(value):
    high = value.astype(jnp.bfloat16)
    return high, (value - high.astype(jnp.float32)).astype(jnp.bfloat16)


def three_pass(left, right, contract=(1, 0)):
    def one(a, b):
        dims = (((contract[0],), (contract[1],)), ((), ()))
        return lax.dot_general(a, b, dims, preferred_element_type=jnp.float32)

    return one(left[0], right[0]) + (one(left[0], right[1]) + one(left[1], right[0]))


def ring_gather_kernel(axis, count, arrays, backward, *refs):
    relayed = backward is not None
    turn, finish = (lambda at: None), (lambda: None)
    if relayed:
        states, refs = refs[:2], refs[2:]
        near, refs = refs[4 * arrays], refs[: 4 * arrays] + refs[4 * arrays + 1 :]
        turn, finish = relay_step(axis, count, backward, (*states, near, *refs[-4:]))
        refs = refs[:-4]
    shards, lefts, outs, products, holds = (
        refs[at * arrays : (at + 1) * arrays] for at in range(5)
    )
    send_sem, recv_sem, store_sem, own_sem = refs[5 * arrays :]
    me, place, right, left = ring_neighbours(axis, count, relayed)
    stores = []

    def product(j, block, region):
        return three_pass(halves(lefts[j][region, :]), halves(block[...]), (0, 0))

    flights = {}
    for step in range(count):
        for j in range(arrays):
            rows = shards[j].shape[0]
            pieces = piece_count(rows // 2, arrays)
            length = rows // 2 // pieces
            for piece in range(pieces):
                for way, sign, target in ((0, -1, right), (1, 1, left)):
                    origin = ring_index(place + sign * step, count)
                    within = (way * pieces + piece) * length
                    region = pl.ds(pl.multiple_of(origin * rows + within, 8), length)
                    if step:
                        flights[step - 1, j, piece, way].wait_recv()
                        source = holds[j].at[region]
                    else:
                        source = shards[j].at[pl.ds(within, length)]
                    if step < count - 1:
                        flight = pltpu.make_async_remote_copy(
                            src_ref=source,
                            dst_ref=holds[j].at[region],
                            send_sem=send_sem.at[way, j + piece, step],
                            recv_sem=recv_sem.at[way, j + piece, step],
                            device_id={axis: target},
                            device_id_type=pl.DeviceIdType.MESH,
                        )
                        flights[step, j, piece, way] = flight
                        flight.start()
                    if step:
                        store = pltpu.make_async_copy(
                            source, outs[j].at[region], store_sem.at[way, j + piece, step - 1]
                        )
                        stores.append(store)
                        store.start()
                        products[j][...] += product(j, source, region)
        if step == 0:
            for j in range(arrays):
                rows = shards[j].shape[0]
                region = pl.ds(pl.multiple_of(me * rows, 8), rows)
                store = pltpu.make_async_copy(shards[j], outs[j].at[region], own_sem.at[j])
                stores.append(store)
                store.start()
                products[j][...] = product(j, shards[j], region)
        if step < count - 1:
            turn(step)
    finish()
    for store in stores:
        store.wait()
    for flight in flights.values():
        flight.wait_send()


def busy_cost(sent):
    return pl.CostEstimate(flops=6000 * sent, bytes_accessed=2 * sent, transcendentals=0)


def ring_gather(shards, lefts, axis, collective_id, relay=None):
    count = lax.axis_size(axis)
    arrays = len(shards)
    states, near, relay_scratch = relay_parts(relay)
    backward = None if relay is None else relay[2]
    sent = sum(shard.size for shard in shards) * 4 * (count - 1)
    whole = [(count * shard.shape[0], shard.shape[1]) for shard in shards]
    return pl.pallas_call(
        functools.partial(ring_gather_kernel, axis, count, arrays, backward),
        out_shape=[jax.ShapeDtypeStruct(shape, jnp.float32) for shape in whole]
        + [
            jax.ShapeDtypeStruct((left.shape[1], shard.shape[1]), jnp.float32)
            for left, shard in zip(lefts, shards)
        ]
        + near,
        in_specs=[pl.BlockSpec(memory_space=pltpu.VMEM)] * (2 * arrays + len(states)),
        out_specs=[pl.BlockSpec(memory_space=pl.ANY)] * arrays
        + [pl.BlockSpec(memory_space=pltpu.VMEM)] * (arrays + len(near)),
        scratch_shapes=[pltpu.VMEM(shape, jnp.float32) for shape in whole]
        + [
            pltpu.SemaphoreType.DMA((2, max(arrays, 2), count - 1)),
            pltpu.SemaphoreType.DMA((2, max(arrays, 2), count - 1)),
            pltpu.SemaphoreType.DMA((2, max(arrays, 2), count - 1)),
            pltpu.SemaphoreType.DMA((arrays,)),
        ]
        + relay_scratch,
        compiler_params=pltpu.CompilerParams(collective_id=collective_id, has_side_effects=True),
        cost_estimate=busy_cost(sent),
        name=f"ring_gather_{collective_id}",
    )(*states, *shards, *lefts)


def ring_scatter_kernel(axis, count, arrays, backward, *refs):
    relayed = backward is not None
    turn, finish = (lambda at: None), (lambda: None)
    if relayed:
        states, refs = refs[:2], refs[2:]
        near, refs = refs[3 * arrays], refs[: 3 * arrays] + refs[3 * arrays + 1 :]
        turn, finish = relay_step(axis, count, backward, (*states, near, *refs[-4:]))
        refs = refs[:-4]
    lefts, rights, outs, slots, firsts, highs, lows = (
        refs[at * arrays : (at + 1) * arrays] for at in range(7)
    )
    send_sem, recv_sem = refs[7 * arrays :]
    for j in range(arrays):
        highs[j][...], lows[j][...] = halves(rights[j][...])
    me, place, right, left = ring_neighbours(axis, count, relayed)
    flights = {}
    for step in range(count):
        for j in range(arrays):
            rows = outs[j].shape[0]
            pieces = piece_count(rows // 2, arrays)
            length = rows // 2 // pieces
            for piece in range(pieces):
                part = pl.ds(piece * length, length)
                for way, sign, target in ((0, -1, right), (1, 1, left)):
                    goal = ring_index(place + sign * (1 + step), count)
                    within = (way * pieces + piece) * length
                    region = pl.ds(pl.multiple_of(goal * rows + within, 8), length)
                    block = three_pass(
                        halves(lefts[j][region, :]), (highs[j][...], lows[j][...])
                    )
                    if step:
                        flights[step - 1, j, piece, way].wait_recv()
                        total = slots[j][way, step - 1, part, :] + block
                        if step == count - 1:
                            outs[j][pl.ds(within, length), :] = total
                            continue
                        slots[j][way, step - 1, part, :] = total
                        source = slots[j].at[way, step - 1, part]
                    else:
                        firsts[j][way, part, :] = block
                        source = firsts[j].at[way, part]
                    flight = pltpu.make_async_remote_copy(
                        src_ref=source,
                        dst_ref=slots[j].at[way, step, part],
                        send_sem=send_sem.at[way, j + piece, step],
                        recv_sem=recv_sem.at[way, j + piece, step],
                        device_id={axis: target},
                        device_id_type=pl.DeviceIdType.MESH,
                    )
                    flights[step, j, piece, way] = flight
                    flight.start()
        if step < count - 1:
            turn(step)
    finish()
    for flight in flights.values():
        flight.wait_send()


def ring_scatter(factors, axis, collective_id, relay=None):
    count = lax.axis_size(axis)
    arrays = len(factors)
    states, near, relay_scratch = relay_parts(relay)
    backward = None if relay is None else relay[2]
    shapes = [(left.shape[0] // count, right.shape[1]) for left, right in factors]
    sent = sum(rows * columns for rows, columns in shapes) * 4 * count
    return pl.pallas_call(
        functools.partial(ring_scatter_kernel, axis, count, arrays, backward),
        out_shape=[jax.ShapeDtypeStruct(shape, jnp.float32) for shape in shapes] + near,
        in_specs=[pl.BlockSpec(memory_space=pltpu.VMEM)] * (2 * arrays + len(states)),
        out_specs=[pl.BlockSpec(memory_space=pltpu.VMEM)] * (arrays + len(near)),
        scratch_shapes=[
            pltpu.VMEM((2, count - 1, rows // 2, columns), jnp.float32) for rows, columns in shapes
        ]
        + [pltpu.VMEM((2, rows // 2, columns), jnp.float32) for rows, columns in shapes]
        + [pltpu.VMEM(right.shape, jnp.bfloat16) for _, right in factors] * 2
        + [
            pltpu.SemaphoreType.DMA((2, max(arrays, 2), count - 1)),
            pltpu.SemaphoreType.DMA((2, max(arrays, 2), count - 1)),
        ]
        + relay_scratch,
        compiler_params=pltpu.CompilerParams(collective_id=collective_id, has_side_effects=True),
        cost_estimate=busy_cost(sent),
        name=f"ring_scatter_{collective_id}",
    )(*states, *[left for left, _ in factors], *[right for _, right in factors])


def silu_grad(pre_value):
    sigmoid_val = jax.nn.sigmoid(pre_value)
    return sigmoid_val * (1.0 + pre_value * (1.0 - sigmoid_val))


def project(activation, weight):
    return jnp.einsum("std,dk->stk", activation, weight, precision=PRECISE)


def back_project(upstream, weight):
    return jnp.einsum("stk,dk->std", upstream, weight, precision=PRECISE)


def weight_grad(activation, upstream):
    return jnp.einsum("std,stk->dk", activation, upstream, precision=PRECISE)


def place_slice(portion, full_size, offset, along):
    full_shape = list(portion.shape)
    full_shape[along] = full_size
    return lax.dynamic_update_slice_in_dim(
        jnp.zeros(full_shape, jnp.float32), portion, offset, along
    )


def running_decay(log_decay):
    seq_count, tokens, head_count = log_decay.shape
    blocks = tokens // GROUP
    grouped = log_decay.reshape(seq_count, blocks, GROUP, head_count)
    rows_at = lax.broadcasted_iota(jnp.int32, (GROUP, GROUP), 0)
    cols_at = lax.broadcasted_iota(jnp.int32, (GROUP, GROUP), 1)
    lower_mask = rows_at >= cols_at
    within = jnp.einsum("ij,sbjh->sbih", lower_mask.astype(jnp.float32), grouped, precision=PRECISE)
    group_total = within[:, :, -1, :]
    through = jnp.cumsum(group_total, axis=1)
    before = through - group_total
    return (lower_mask, within, group_total, through, before)


def group_core(values, step_size, log_decay, b_state, c_state, skip_gain):
    seq_count, tokens, width = values.shape
    head_count = step_size.shape[2]
    head_dim = width // head_count
    blocks = tokens // GROUP
    lower_mask, within, group_total, through, before = running_decay(log_decay)
    head_values = values.reshape(seq_count, blocks, GROUP, head_count, head_dim)
    step_blocks = step_size.reshape(seq_count, blocks, GROUP, head_count)
    b_blocks = b_state.reshape(seq_count, blocks, GROUP, -1)
    c_blocks = c_state.reshape(seq_count, blocks, GROUP, -1)
    decay_rows = within.transpose(0, 1, 3, 2)
    log_gaps = decay_rows[..., :, None] - decay_rows[..., None, :]
    decay_mat = jnp.where(lower_mask, jnp.exp(jnp.where(lower_mask, log_gaps, 0.0)), 0.0)
    scores = jnp.einsum("sbin,sbjn->sbij", c_blocks, b_blocks, precision=PRECISE)
    weighted = scores[:, :, None] * decay_mat * step_blocks.transpose(0, 1, 3, 2)[:, :, :, None, :]
    intra_out = jnp.einsum("sbhij,sbjhp->sbihp", weighted, head_values, precision=PRECISE)
    to_end = jnp.exp(group_total[:, :, None, :] - within) * step_blocks
    states = jnp.einsum("sbjh,sbjhp,sbjn->sbhpn", to_end, head_values, b_blocks, precision=PRECISE)
    later_at = lax.broadcasted_iota(jnp.int32, (blocks, blocks), 0)
    earlier_at = lax.broadcasted_iota(jnp.int32, (blocks, blocks), 1)
    earlier_mask = (later_at > earlier_at)[None, :, :, None]
    carry_gap = before[:, :, None, :] - through[:, None, :, :]
    carry_factor = jnp.where(earlier_mask, jnp.exp(jnp.where(earlier_mask, carry_gap, 0.0)), 0.0)
    entering = jnp.einsum("skmh,smhpn->skhpn", carry_factor, states, precision=PRECISE)
    inter_out = (
        jnp.einsum("sbin,sbhpn->sbihp", c_blocks, entering, precision=PRECISE)
        * jnp.exp(within)[..., None]
    )
    output = intra_out + inter_out + skip_gain[:, None] * head_values
    end_gap = through - through
    summary = jnp.einsum("sbh,sbhpn->shpn", jnp.exp(end_gap), states, precision=PRECISE)
    decay_all = jnp.exp(through[:, -1, :])
    return (output.reshape(seq_count, tokens, width), decay_all, summary)


def entry_term(entry_state, log_decay, c_state):
    seq_count, tokens, head_count = log_decay.shape
    blocks = tokens // GROUP
    _, within, _, _, before = running_decay(log_decay)
    reach = jnp.exp(within + before[:, :, None, :])
    c_blocks = c_state.reshape(seq_count, blocks, GROUP, -1)
    result = (
        jnp.einsum("sbin,shpn->sbihp", c_blocks, entry_state, precision=PRECISE) * reach[..., None]
    )
    return result.reshape(seq_count, tokens, -1)


def full_mixer(values, step_size, log_decay, b_state, c_state, skip_gain, entry_state):
    base_out, decay_all, summary = group_core(
        values, step_size, log_decay, b_state, c_state, skip_gain
    )
    output = base_out + entry_term(entry_state, log_decay, c_state)
    leaving = decay_all[..., None, None] * entry_state + summary
    return (output, leaving)


def gram_strips(rows):
    size = rows.shape[1]
    block = min(size, 256)
    return [
        jnp.einsum("ri,rj->ij", rows[:, at : at + block], rows[:, at:], precision=PRECISE)
        for at in range(0, size, block)
    ]


def orthogonal_kernel(arrays, strip_counts, *refs):

    grams = []
    for strips in strip_counts:
        grams.append(refs[:strips])
        refs = refs[strips:]
    rows, outs, scratch = refs[:arrays], refs[arrays : 2 * arrays], refs[2 * arrays :]
    work = [scratch[8 * j : 8 * j + 8] for j in range(arrays)]
    for j in range(arrays):
        whole = work[j][0]
        block = grams[j][0].shape[0]
        spots = [slice(at * block, (at + 1) * block) for at in range(len(grams[j]))]
        across = lax.broadcasted_iota(jnp.int32, (block, block), 0)
        down = lax.broadcasted_iota(jnp.int32, (block, block), 1)
        total = jnp.zeros((1, 1), jnp.float32)
        for strip in grams[j]:
            diagonal = jnp.where(across == down, strip[:, :block], 0.0)
            total += jnp.sum(jnp.sum(diagonal, axis=0, keepdims=True), axis=1, keepdims=True)
        factor = 1.0 / (jnp.sqrt(total) + 1e-07)
        square = factor * factor
        for i, strip in enumerate(grams[j]):
            for k in range(i, len(spots)):
                piece = strip[:, (k - i) * block : (k - i + 1) * block] * square
                whole[spots[i], spots[k]] = piece
                if i != k:
                    whole[spots[k], spots[i]] = piece.T
        outs[j][...] = rows[j][...] * factor

    def split_whole(j, at):
        whole, high, low = work[j][0], work[j][1], work[j][2]
        high[at, :], low[at, :] = halves(whole[at, :])

    def sweep(last):
        strips = []
        for j in range(arrays):
            size = rows[j].shape[1]
            strip = min(size, 256)
            strips.append([slice(s, s + strip) for s in range(0, size, strip)])
        for j in range(arrays):
            for at in strips[j]:
                split_whole(j, at)
        for j in range(arrays):
            whole, high, low, poly_h, poly_l, _, _, _ = work[j]
            for at in strips[j]:
                poly = QUINTIC_B * whole[at, :] + QUINTIC_C * three_pass(
                    (high[at, :], low[at, :]), (high[...], low[...])
                )
                poly_h[at, :], poly_l[at, :] = halves(poly)
        for j in range(arrays):
            poly = (work[j][3][...], work[j][4][...])
            value = outs[j][...]
            outs[j][...] = QUINTIC_A * value + three_pass(halves(value), poly)
        if last:
            return
        for j in range(arrays):
            whole, high, low, poly_h, poly_l, half, half_h, half_l = work[j]
            for at in strips[j]:
                value = QUINTIC_A * whole[at, :] + three_pass(
                    (poly_h[at, :], poly_l[at, :]), (high[...], low[...])
                )
                half[at, :] = value
                half_h[at, :], half_l[at, :] = halves(value)
        for j in range(arrays):
            whole, _, _, poly_h, poly_l, half, half_h, half_l = work[j]
            for at in strips[j]:
                whole[at, :] = QUINTIC_A * half[at, :] + three_pass(
                    (half_h[at, :], half_l[at, :]), (poly_h[...], poly_l[...])
                )

    def body(_, carry):
        sweep(False)
        return carry

    lax.fori_loop(0, SWEEPS - 1, body, 0)
    sweep(True)


def orthogonal_rows(pairs, name):
    arrays = len(pairs)
    scratch = []
    flops = 0
    for _, rows in pairs:
        size = rows.shape[1]
        full, narrow = pltpu.VMEM((size, size), jnp.float32), pltpu.VMEM((size, size), jnp.bfloat16)
        scratch += [full, narrow, narrow, narrow, narrow, full, narrow, narrow]
        flops += 6 * (13 * size**3 + 5 * rows.shape[0] * size**2)
    return pl.pallas_call(
        functools.partial(orthogonal_kernel, arrays, [len(strips) for strips, _ in pairs]),
        out_shape=[jax.ShapeDtypeStruct(rows.shape, jnp.float32) for _, rows in pairs],
        in_specs=[pl.BlockSpec(memory_space=pltpu.VMEM)]
        * (arrays + sum(len(strips) for strips, _ in pairs)),
        out_specs=[pl.BlockSpec(memory_space=pltpu.VMEM)] * arrays,
        scratch_shapes=scratch,
        cost_estimate=pl.CostEstimate(flops=flops, bytes_accessed=0, transcendentals=0),
        name=name,
    )(*[strip for strips, _ in pairs for strip in strips], *[rows for _, rows in pairs])


def on_device(
    block_input,
    cotangent,
    gate_proj,
    value_proj,
    bc_proj,
    step_proj,
    out_proj,
    in_gain,
    conv_value,
    conv_bc,
    head_params,
    out_gain,
    m_gate,
    m_value,
    m_bc,
    m_step,
    m_out,
    m_ingain,
    m_convvalue,
    m_convbc,
    m_head,
    m_outgain,
):
    head_count = lax.axis_size("head")
    head_index = lax.axis_index("head")
    seq_count, tokens, _ = block_input.shape
    row_count = gate_proj.shape[0]
    inner_width = gate_proj.shape[1]
    local_heads = step_proj.shape[1]
    bc_width = 2 * STATE // head_count
    model_part = D // head_count
    side_width = -(-(bc_width + local_heads) // LANES) * LANES
    bc_cols_mine = lax.dynamic_slice_in_dim(bc_proj, head_index * bc_width, bc_width, 1)
    side_mine = jnp.concatenate(
        [
            value_proj,
            bc_cols_mine,
            step_proj,
            jnp.zeros((row_count, side_width - bc_width - local_heads), jnp.float32),
        ],
        axis=1,
    )
    conv_mine = lax.dynamic_slice_in_dim(conv_value, head_index * inner_width, inner_width, 1)
    gain_mine = lax.dynamic_slice_in_dim(out_gain, head_index * inner_width, inner_width, 0)
    head_mine = lax.dynamic_slice_in_dim(head_params, head_index * local_heads, local_heads, 1)
    bc_taps = lax.dynamic_slice_in_dim(conv_bc, head_index * bc_width, bc_width, 1)
    inv_rms = lax.rsqrt(jnp.mean(block_input * block_input, axis=-1, keepdims=True) + EPSILON)
    normed = block_input * inv_rms * in_gain
    normed_turned = normed[0].T
    cotangent_turned = cotangent[0].T
    mixed_full, all_pre = ring_gather((side_mine,), (normed_turned,), "seq", 0)
    all_pre = all_pre[None]
    mixed_width = inner_width + bc_width
    mixed_pre = all_pre[..., :mixed_width]
    step_pre = all_pre[..., mixed_width : mixed_width + local_heads]
    conv_taps = jnp.concatenate([conv_mine, bc_taps], axis=-1)
    edge_rows = from_behind(mixed_pre[:, tokens - (CONV - 1) :, :], "seq", 1)
    padded = jnp.concatenate([edge_rows, mixed_pre], axis=1)
    conv_out = conv_taps[CONV] + sum(
        (conv_taps[offset] * padded[:, offset : offset + tokens, :] for offset in range(CONV))
    )
    activated = jax.nn.silu(conv_out)
    values = activated[..., :inner_width]
    bc_all = lax.all_gather(activated[..., inner_width:], "head", axis=2, tiled=True)
    b_state = bc_all[..., :STATE]
    c_state = bc_all[..., STATE:]
    decay_rate = jnp.exp(head_mine[0])
    skip_gain = head_mine[1]
    step_arg = step_pre + head_mine[2]
    step_size = jax.nn.softplus(step_arg)
    log_decay = -decay_rate * step_size
    base_out, decay_all, summary = group_core(
        values, step_size, log_decay, b_state, c_state, skip_gain
    )
    state_shape = summary.shape
    state_rows = (-1, state_shape[-1])
    decay_rows = jnp.broadcast_to(decay_all[..., None, None], state_shape).reshape(state_rows)
    gate_full, out_full, gate_pre, grad_normout, entry_rows = ring_gather(
        (gate_proj, out_proj.T),
        (normed_turned, cotangent_turned),
        "seq",
        1,
        (summary.reshape(state_rows), decay_rows, False),
    )
    gate_pre, grad_normout = gate_pre[None], grad_normout[None]
    entry_state = entry_rows.reshape(state_shape)
    mixer_out = base_out + entry_term(entry_state, log_decay, c_state)
    gate_act = jax.nn.silu(gate_pre)
    gated = mixer_out * gate_act
    square_part = jnp.sum(gated * gated, axis=-1, keepdims=True)
    out_part = back_project(gated * gain_mine, out_full)
    out_sum = lax.psum_scatter(out_part, "head", scatter_dimension=2, tiled=True)
    scaled = grad_normout * gain_mine
    dot_part = jnp.sum(scaled * gated, axis=-1, keepdims=True)
    square_sum, dot_total = lax.psum((square_part, dot_part), "head")
    gate_rms = lax.rsqrt(square_sum / DI + EPSILON)
    input_mine = lax.dynamic_slice_in_dim(block_input, head_index * model_part, model_part, 2)
    cotangent_mine = lax.dynamic_slice_in_dim(cotangent, head_index * model_part, model_part, 2)
    normed_out = gated * gate_rms * gain_mine
    grad_outgain_mine = jnp.sum(grad_normout * gated * gate_rms, axis=(0, 1))
    grad_gated = gate_rms * scaled - gate_rms**3 * gated * dot_total / DI
    grad_mixer = grad_gated * gate_act
    grad_gate_pre = grad_gated * mixer_out * silu_grad(gate_pre)
    _, entry_back = jax.vjp(lambda entering: entry_term(entering, log_decay, c_state), entry_state)
    direct = entry_back(grad_mixer)[0]
    grad_out_rows, grad_gate, leave_rows = ring_scatter(
        ((cotangent_turned, normed_out[0]), (normed_turned, grad_gate_pre[0])),
        "seq",
        2,
        (direct.reshape(state_rows), decay_rows, True),
    )
    leave_rows, out_sum = lax.optimization_barrier((leave_rows, out_sum))
    block_output = input_mine + gate_rms * out_sum
    leave_grad = leave_rows.reshape(state_shape)
    _, mixer_back = jax.vjp(
        full_mixer, values, step_size, log_decay, b_state, c_state, skip_gain, entry_state
    )
    grad_values, grad_stepsize, grad_logdecay, grad_b, grad_c, grad_skip, _ = mixer_back(
        (grad_mixer, leave_grad)
    )
    grad_step_total = grad_stepsize - grad_logdecay * decay_rate
    grad_alog = jnp.sum(grad_logdecay * log_decay, axis=(0, 1))
    grad_step_pre = grad_step_total * jax.nn.sigmoid(step_arg)
    grad_bias = jnp.sum(grad_step_pre, axis=(0, 1))
    grad_bc_all = jnp.concatenate([grad_b, grad_c], axis=-1)
    grad_bc_act = lax.psum_scatter(grad_bc_all, "head", scatter_dimension=2, tiled=True)
    grad_conv = jnp.concatenate([grad_values, grad_bc_act], axis=-1) * silu_grad(conv_out)
    grad_taps = jnp.stack(
        [
            jnp.sum(grad_conv * padded[:, offset : offset + tokens, :], axis=(0, 1))
            for offset in range(CONV)
        ]
        + [jnp.sum(grad_conv, axis=(0, 1))]
    )
    grad_padded = sum(
        (
            jnp.pad(conv_taps[offset] * grad_conv, ((0, 0), (offset, CONV - 1 - offset), (0, 0)))
            for offset in range(CONV)
        )
    )
    edge_back = from_behind(grad_padded[:, : CONV - 1, :], "seq", -1)
    grad_mixed = grad_padded[:, CONV - 1 :, :] + jnp.pad(
        edge_back, ((0, 0), (tokens - (CONV - 1), 0), (0, 0))
    )
    grad_all_pre = jnp.concatenate(
        [
            grad_mixed,
            grad_step_pre,
            jnp.zeros((seq_count, tokens, side_width - bc_width - local_heads), jnp.float32),
        ],
        axis=-1,
    )
    grad_normed = back_project(grad_gate_pre, gate_full) + back_project(grad_all_pre, mixed_full)
    stat_part = jnp.sum(grad_normed * in_gain * block_input, axis=-1, keepdims=True)
    grad_ingain_part = jnp.sum(grad_normed * block_input * inv_rms, axis=(0, 1))
    (grad_mixed_rows,) = ring_scatter(((normed_turned, grad_all_pre[0]),), "seq", 3)
    grad_value = grad_mixed_rows[:, :inner_width]
    grad_bc = lax.all_gather(
        grad_mixed_rows[:, inner_width:mixed_width], "head", axis=1, tiled=True
    )
    grad_step = grad_mixed_rows[:, mixed_width : mixed_width + local_heads]
    grad_out = grad_out_rows.T
    next_out_rows = MOMENTUM_KEEP * m_out.T + grad_out_rows
    next_gate = MOMENTUM_KEEP * m_gate + grad_gate
    next_value = MOMENTUM_KEEP * m_value + grad_value
    next_bc = MOMENTUM_KEEP * m_bc + grad_bc
    next_step = MOMENTUM_KEEP * m_step + grad_step
    next_out = MOMENTUM_KEEP * m_out + grad_out
    pieces = (
        grad_ingain_part,
        grad_taps.reshape(-1),
        grad_alog,
        grad_skip,
        grad_bias,
        grad_outgain_mine,
    )
    flat = jnp.concatenate(pieces)
    flat_rows = -(-flat.shape[0] // (16 * STATE)) * 8
    flat = jnp.pad(flat, (0, flat_rows * 2 * STATE - flat.shape[0])).reshape(flat_rows, 2 * STATE)
    side = 2 * STATE
    strips = len(gram_strips(next_gate))
    early = lax.psum(gram_strips(next_out_rows) + gram_strips(next_gate), "seq")
    out_gram, gate_gram = early[:strips], early[strips:]
    late_value, _ = lax.optimization_barrier((next_value, early))
    (step_gram,) = gram_strips(next_step)
    step_gram = jnp.pad(step_gram, ((0, -local_heads % 8), (0, side - local_heads)))
    late = lax.psum(
        gram_strips(late_value)
        + [jnp.concatenate(gram_strips(next_bc) + [step_gram, flat], axis=0)],
        "seq",
    )
    value_gram, side_gram = late[:-1], late[-1]
    flat = side_gram[side + step_gram.shape[0] :]
    step_gram = jnp.pad(
        side_gram[side : side + step_gram.shape[0], :LANES],
        ((0, LANES - step_gram.shape[0]), (0, 0)),
    )
    flat = lax.all_gather(flat, "head").reshape(head_count, flat_rows * 2 * STATE)
    parts = []
    start = 0
    for piece in pieces:
        parts.append(flat[:, start : start + piece.shape[0]])
        start += piece.shape[0]
    grad_ingain = jnp.sum(parts[0], axis=0)
    taps_all = parts[1].reshape(head_count, CONV + 1, mixed_width)
    grad_convvalue = taps_all[:, :, :inner_width].transpose(1, 0, 2).reshape(CONV + 1, DI)
    grad_convbc = taps_all[:, :, inner_width:].transpose(1, 0, 2).reshape(CONV + 1, 2 * STATE)
    grad_head = jnp.stack([parts[2].reshape(H), parts[3].reshape(H), parts[4].reshape(H)])
    grad_outgain = parts[5].reshape(DI)
    next_ingain = MOMENTUM_KEEP * m_ingain + grad_ingain
    next_convvalue = MOMENTUM_KEEP * m_convvalue + grad_convvalue
    next_convbc = MOMENTUM_KEEP * m_convbc + grad_convbc
    next_head = MOMENTUM_KEEP * m_head + grad_head
    next_outgain = MOMENTUM_KEEP * m_outgain + grad_outgain
    update_out, update_gate = orthogonal_rows(
        ((out_gram, next_out_rows), (gate_gram, next_gate)), "ortho_first"
    )
    grad_normed, stat_part, update_out = lax.optimization_barrier(
        (grad_normed, stat_part, update_out)
    )
    update_out = update_out.T
    normed_grad_mine = lax.psum_scatter(grad_normed, "head", scatter_dimension=2, tiled=True)
    stat_total = lax.psum(stat_part, "head")
    gain_part = lax.dynamic_slice_in_dim(in_gain, head_index * model_part, model_part, 0)
    input_grad = (
        cotangent_mine
        + inv_rms * gain_part * normed_grad_mine
        - inv_rms**3 * input_mine * stat_total / D
    )
    update_value, update_bc, update_step = orthogonal_rows(
        (
            (value_gram, next_value),
            ([side_gram[:side]], next_bc),
            ([step_gram], jnp.pad(next_step, ((0, 0), (0, LANES - local_heads)))),
        ),
        "ortho_last",
    )
    update_step = update_step[:, :local_heads]
    update_scale = MATRIX_RATE * MUON_SCALE * math.sqrt(D)
    new_gate = gate_proj - update_scale * update_gate
    new_value = value_proj - update_scale * update_value
    new_bc = bc_proj - update_scale * update_bc
    new_step = step_proj - update_scale * update_step
    new_out = out_proj - update_scale * update_out
    new_ingain = in_gain - VECTOR_RATE * next_ingain
    new_convvalue = conv_value - VECTOR_RATE * next_convvalue
    new_convbc = conv_bc - VECTOR_RATE * next_convbc
    new_head = head_params - VECTOR_RATE * next_head
    new_outgain = out_gain - VECTOR_RATE * next_outgain
    return (
        block_output,
        input_grad,
        grad_gate,
        grad_value,
        grad_bc,
        grad_step,
        grad_out,
        grad_ingain,
        grad_convvalue,
        grad_convbc,
        grad_head,
        grad_outgain,
        new_gate,
        new_value,
        new_bc,
        new_step,
        new_out,
        new_ingain,
        new_convvalue,
        new_convbc,
        new_head,
        new_outgain,
        next_gate,
        next_value,
        next_bc,
        next_step,
        next_out,
        next_ingain,
        next_convvalue,
        next_convbc,
        next_head,
        next_outgain,
    )


def solution(mesh):
    in_specs = (
        P(None, "seq", None),
        P(None, "seq", None),
        P("seq", "head"),
        P("seq", "head"),
        P("seq", None),
        P("seq", "head"),
        P("head", "seq"),
        P(),
        P(),
        P(),
        P(),
        P(),
        P("seq", "head"),
        P("seq", "head"),
        P("seq", None),
        P("seq", "head"),
        P("head", "seq"),
        P(),
        P(),
        P(),
        P(),
        P(),
    )
    out_specs = (
        P(None, "seq", "head"),
        P(None, "seq", "head"),
        P("seq", "head"),
        P("seq", "head"),
        P("seq", None),
        P("seq", "head"),
        P("head", "seq"),
        P(),
        P(),
        P(),
        P(),
        P(),
        P("seq", "head"),
        P("seq", "head"),
        P("seq", None),
        P("seq", "head"),
        P("head", "seq"),
        P(),
        P(),
        P(),
        P(),
        P(),
        P("seq", "head"),
        P("seq", "head"),
        P("seq", None),
        P("seq", "head"),
        P("head", "seq"),
        P(),
        P(),
        P(),
        P(),
        P(),
    )
    return jax.shard_map(
        on_device, mesh=mesh, in_specs=in_specs, out_specs=out_specs, check_vma=False
    )
```

```python
import functools
import math

import jax
import jax.numpy as jnp
from jax import lax
from jax.experimental import pallas as pl
from jax.experimental.pallas import tpu as pltpu
from jax.sharding import PartitionSpec as P

D = 1536
DI = 3072
STATE = 128
H = 48
GROUP = 256
CONV = 4
SWEEPS = 5


PRECISE = lax.Precision.HIGH
EPSILON = 1e-05
QUINTIC_A = 3.4445
QUINTIC_B = -4.775
QUINTIC_C = 2.0315
MOMENTUM_KEEP = 0.9
MATRIX_RATE = 0.02
VECTOR_RATE = 0.002
MUON_SCALE = 0.2


LANES = 128


def from_behind(value, axis, steps):
    count = lax.axis_size(axis)
    initial, last = (max(0, -steps), min(count, count - steps))
    return lax.ppermute(value, axis, [(source, source + steps) for source in range(initial, last)])


def ring_place(index, count):
    odd = index % 2
    return (1 - odd) * (index // 2) + odd * (count - 1 - index // 2)


def ring_index(position, count):
    position = (position + 2 * count) % count
    back = position // (count // 2)
    return (1 - back) * (2 * position) + back * (2 * (count - 1 - position) + 1)


def greet(axis, neighbours):
    barrier = pltpu.get_barrier_semaphore()
    for neighbour in neighbours:
        pl.semaphore_signal(
            barrier, inc=1, device_id={axis: neighbour}, device_id_type=pl.DeviceIdType.MESH
        )
    pl.semaphore_wait(barrier, len(neighbours))


def piece_count(half, arrays):
    return 2 if arrays == 1 and half % 16 == 0 else 1


def relay_step(axis, count, backward, refs):
    own, decay, near, entering, leaving, send_sem, recv_sem = refs
    me = lax.axis_index(axis)
    order = count - 1 - me if backward else me
    ahead = (me + count - 1) % count if backward else (me + 1) % count
    copy = pltpu.make_async_remote_copy(
        src_ref=leaving,
        dst_ref=entering,
        send_sem=send_sem,
        recv_sem=recv_sem,
        device_id={axis: ahead},
        device_id_type=pl.DeviceIdType.MESH,
    )

    def turn(at):
        @pl.when(order == at)
        def _():
            if at:
                copy.wait_recv()
                near[...] = entering[...]
                if at < count - 1:
                    leaving[...] = own[...] + decay[...] * entering[...]
            else:
                near[...] = jnp.zeros_like(near)
                leaving[...] = own[...]
            if at < count - 1:
                copy.start()

    def finish():
        turn(count - 1)

        @pl.when(order < count - 1)
        def _():
            copy.wait_send()

    return turn, finish


def relay_parts(relay):
    if relay is None:
        return [], [], []
    state = relay[0]
    buffers = [pltpu.VMEM(state.shape, state.dtype)] * 2
    return (
        [relay[0], relay[1]],
        [jax.ShapeDtypeStruct(state.shape, state.dtype)],
        buffers + [pltpu.SemaphoreType.DMA(()), pltpu.SemaphoreType.DMA(())],
    )


def ring_neighbours(axis, count, relayed):
    me = lax.axis_index(axis)
    place = ring_place(me, count)
    right, left = ring_index(place + 1, count), ring_index(place - 1, count)
    greeted = (left, right)
    if relayed:
        greeted += ((me + 1) % count, (me + count - 1) % count)
    greet(axis, greeted)
    return me, place, right, left


def halves(value):
    high = value.astype(jnp.bfloat16)
    return high, (value - high.astype(jnp.float32)).astype(jnp.bfloat16)


def three_pass(left, right, contract=(1, 0)):
    def one(a, b):
        dims = (((contract[0],), (contract[1],)), ((), ()))
        return lax.dot_general(a, b, dims, preferred_element_type=jnp.float32)

    return one(left[0], right[0]) + (one(left[0], right[1]) + one(left[1], right[0]))


def ring_gather_kernel(axis, count, arrays, backward, *refs):
    relayed = backward is not None
    turn, finish = (lambda at: None), (lambda: None)
    if relayed:
        states, refs = refs[:2], refs[2:]
        near, refs = refs[4 * arrays], refs[: 4 * arrays] + refs[4 * arrays + 1 :]
        turn, finish = relay_step(axis, count, backward, (*states, near, *refs[-4:]))
        refs = refs[:-4]
    shards, lefts, outs, products, holds = (
        refs[at * arrays : (at + 1) * arrays] for at in range(5)
    )
    send_sem, recv_sem, store_sem, own_sem = refs[5 * arrays :]
    me, place, right, left = ring_neighbours(axis, count, relayed)
    stores = []

    def product(j, block, region):
        return three_pass(halves(lefts[j][region, :]), halves(block[...]), (0, 0))

    flights = {}
    for step in range(count):
        for j in range(arrays):
            rows = shards[j].shape[0]
            pieces = piece_count(rows // 2, arrays)
            length = rows // 2 // pieces
            for piece in range(pieces):
                for way, sign, target in ((0, -1, right), (1, 1, left)):
                    origin = ring_index(place + sign * step, count)
                    within = (way * pieces + piece) * length
                    region = pl.ds(pl.multiple_of(origin * rows + within, 8), length)
                    if step:
                        flights[step - 1, j, piece, way].wait_recv()
                        source = holds[j].at[region]
                    else:
                        source = shards[j].at[pl.ds(within, length)]
                    if step < count - 1:
                        flight = pltpu.make_async_remote_copy(
                            src_ref=source,
                            dst_ref=holds[j].at[region],
                            send_sem=send_sem.at[way, j + piece, step],
                            recv_sem=recv_sem.at[way, j + piece, step],
                            device_id={axis: target},
                            device_id_type=pl.DeviceIdType.MESH,
                        )
                        flights[step, j, piece, way] = flight
                        flight.start()
                    if step:
                        store = pltpu.make_async_copy(
                            source, outs[j].at[region], store_sem.at[way, j + piece, step - 1]
                        )
                        stores.append(store)
                        store.start()
                        products[j][...] += product(j, source, region)
        if step == 0:
            for j in range(arrays):
                rows = shards[j].shape[0]
                region = pl.ds(pl.multiple_of(me * rows, 8), rows)
                store = pltpu.make_async_copy(shards[j], outs[j].at[region], own_sem.at[j])
                stores.append(store)
                store.start()
                products[j][...] = product(j, shards[j], region)
        if step < count - 1:
            turn(step)
    finish()
    for store in stores:
        store.wait()
    for flight in flights.values():
        flight.wait_send()


def busy_cost(sent):
    return pl.CostEstimate(flops=6000 * sent, bytes_accessed=2 * sent, transcendentals=0)


def ring_gather(shards, lefts, axis, collective_id, relay=None):
    count = lax.axis_size(axis)
    arrays = len(shards)
    states, near, relay_scratch = relay_parts(relay)
    backward = None if relay is None else relay[2]
    sent = sum(shard.size for shard in shards) * 4 * (count - 1)
    whole = [(count * shard.shape[0], shard.shape[1]) for shard in shards]
    return pl.pallas_call(
        functools.partial(ring_gather_kernel, axis, count, arrays, backward),
        out_shape=[jax.ShapeDtypeStruct(shape, jnp.float32) for shape in whole]
        + [
            jax.ShapeDtypeStruct((left.shape[1], shard.shape[1]), jnp.float32)
            for left, shard in zip(lefts, shards)
        ]
        + near,
        in_specs=[pl.BlockSpec(memory_space=pltpu.VMEM)] * (2 * arrays + len(states)),
        out_specs=[pl.BlockSpec(memory_space=pl.ANY)] * arrays
        + [pl.BlockSpec(memory_space=pltpu.VMEM)] * (arrays + len(near)),
        scratch_shapes=[pltpu.VMEM(shape, jnp.float32) for shape in whole]
        + [
            pltpu.SemaphoreType.DMA((2, max(arrays, 2), count - 1)),
            pltpu.SemaphoreType.DMA((2, max(arrays, 2), count - 1)),
            pltpu.SemaphoreType.DMA((2, max(arrays, 2), count - 1)),
            pltpu.SemaphoreType.DMA((arrays,)),
        ]
        + relay_scratch,
        compiler_params=pltpu.CompilerParams(collective_id=collective_id, has_side_effects=True),
        cost_estimate=busy_cost(sent),
        name=f"ring_gather_{collective_id}",
    )(*states, *shards, *lefts)


def ring_scatter_kernel(axis, count, arrays, backward, *refs):
    relayed = backward is not None
    turn, finish = (lambda at: None), (lambda: None)
    if relayed:
        states, refs = refs[:2], refs[2:]
        near, refs = refs[3 * arrays], refs[: 3 * arrays] + refs[3 * arrays + 1 :]
        turn, finish = relay_step(axis, count, backward, (*states, near, *refs[-4:]))
        refs = refs[:-4]
    lefts, rights, outs, slots, firsts, highs, lows = (
        refs[at * arrays : (at + 1) * arrays] for at in range(7)
    )
    send_sem, recv_sem = refs[7 * arrays :]
    for j in range(arrays):
        highs[j][...], lows[j][...] = halves(rights[j][...])
    me, place, right, left = ring_neighbours(axis, count, relayed)
    flights = {}
    for step in range(count):
        for j in range(arrays):
            rows = outs[j].shape[0]
            pieces = piece_count(rows // 2, arrays)
            length = rows // 2 // pieces
            for piece in range(pieces):
                part = pl.ds(piece * length, length)
                for way, sign, target in ((0, -1, right), (1, 1, left)):
                    goal = ring_index(place + sign * (1 + step), count)
                    within = (way * pieces + piece) * length
                    region = pl.ds(pl.multiple_of(goal * rows + within, 8), length)
                    block = three_pass(
                        halves(lefts[j][region, :]), (highs[j][...], lows[j][...])
                    )
                    if step:
                        flights[step - 1, j, piece, way].wait_recv()
                        total = slots[j][way, step - 1, part, :] + block
                        if step == count - 1:
                            outs[j][pl.ds(within, length), :] = total
                            continue
                        slots[j][way, step - 1, part, :] = total
                        source = slots[j].at[way, step - 1, part]
                    else:
                        firsts[j][way, part, :] = block
                        source = firsts[j].at[way, part]
                    flight = pltpu.make_async_remote_copy(
                        src_ref=source,
                        dst_ref=slots[j].at[way, step, part],
                        send_sem=send_sem.at[way, j + piece, step],
                        recv_sem=recv_sem.at[way, j + piece, step],
                        device_id={axis: target},
                        device_id_type=pl.DeviceIdType.MESH,
                    )
                    flights[step, j, piece, way] = flight
                    flight.start()
        if step < count - 1:
            turn(step)
    finish()
    for flight in flights.values():
        flight.wait_send()


def ring_scatter(factors, axis, collective_id, relay=None):
    count = lax.axis_size(axis)
    arrays = len(factors)
    states, near, relay_scratch = relay_parts(relay)
    backward = None if relay is None else relay[2]
    shapes = [(left.shape[0] // count, right.shape[1]) for left, right in factors]
    sent = sum(rows * columns for rows, columns in shapes) * 4 * count
    return pl.pallas_call(
        functools.partial(ring_scatter_kernel, axis, count, arrays, backward),
        out_shape=[jax.ShapeDtypeStruct(shape, jnp.float32) for shape in shapes] + near,
        in_specs=[pl.BlockSpec(memory_space=pltpu.VMEM)] * (2 * arrays + len(states)),
        out_specs=[pl.BlockSpec(memory_space=pltpu.VMEM)] * (arrays + len(near)),
        scratch_shapes=[
            pltpu.VMEM((2, count - 1, rows // 2, columns), jnp.float32) for rows, columns in shapes
        ]
        + [pltpu.VMEM((2, rows // 2, columns), jnp.float32) for rows, columns in shapes]
        + [pltpu.VMEM(right.shape, jnp.bfloat16) for _, right in factors] * 2
        + [
            pltpu.SemaphoreType.DMA((2, max(arrays, 2), count - 1)),
            pltpu.SemaphoreType.DMA((2, max(arrays, 2), count - 1)),
        ]
        + relay_scratch,
        compiler_params=pltpu.CompilerParams(collective_id=collective_id, has_side_effects=True),
        cost_estimate=busy_cost(sent),
        name=f"ring_scatter_{collective_id}",
    )(*states, *[left for left, _ in factors], *[right for _, right in factors])


def direct_scatter_kernel(axis, count, parts, out, slots, send_sem, recv_sem):
    me = lax.axis_index(axis)
    greet(axis, [(me + away) % count for away in range(1, count)])
    flights = []
    for away in range(1, count):
        target = (me + away) % count
        flight = pltpu.make_async_remote_copy(
            src_ref=parts.at[target],
            dst_ref=slots.at[away - 1],
            send_sem=send_sem.at[away - 1],
            recv_sem=recv_sem.at[away - 1],
            device_id={axis: target},
            device_id_type=pl.DeviceIdType.MESH,
        )
        flights.append(flight)
        flight.start()
    total = parts[me]
    for away in range(1, count):
        flights[away - 1].wait_recv()
        total = total + slots[away - 1]
    out[...] = total
    for flight in flights:
        flight.wait_send()


def direct_scatter(parts, axis, collective_id):
    count = lax.axis_size(axis)
    shape = parts.shape[1:]
    return pl.pallas_call(
        functools.partial(direct_scatter_kernel, axis, count),
        out_shape=jax.ShapeDtypeStruct(shape, jnp.float32),
        in_specs=[pl.BlockSpec(memory_space=pltpu.VMEM)],
        out_specs=pl.BlockSpec(memory_space=pltpu.VMEM),
        scratch_shapes=[
            pltpu.VMEM((count - 1, *shape), jnp.float32),
            pltpu.SemaphoreType.DMA((count - 1,)),
            pltpu.SemaphoreType.DMA((count - 1,)),
        ],
        compiler_params=pltpu.CompilerParams(collective_id=collective_id, has_side_effects=True),
        name=f"direct_scatter_{collective_id}",
    )(parts)


def silu_grad(pre_value):
    sigmoid_val = jax.nn.sigmoid(pre_value)
    return sigmoid_val * (1.0 + pre_value * (1.0 - sigmoid_val))


def project(activation, weight):
    return jnp.einsum("std,dk->stk", activation, weight, precision=PRECISE)


def back_project(upstream, weight):
    return jnp.einsum("stk,dk->std", upstream, weight, precision=PRECISE)


def weight_grad(activation, upstream):
    return jnp.einsum("std,stk->dk", activation, upstream, precision=PRECISE)


def place_slice(portion, full_size, offset, along):
    full_shape = list(portion.shape)
    full_shape[along] = full_size
    return lax.dynamic_update_slice_in_dim(
        jnp.zeros(full_shape, jnp.float32), portion, offset, along
    )


def running_decay(log_decay):
    seq_count, tokens, head_count = log_decay.shape
    blocks = tokens // GROUP
    grouped = log_decay.reshape(seq_count, blocks, GROUP, head_count)
    rows_at = lax.broadcasted_iota(jnp.int32, (GROUP, GROUP), 0)
    cols_at = lax.broadcasted_iota(jnp.int32, (GROUP, GROUP), 1)
    lower_mask = rows_at >= cols_at
    within = jnp.einsum("ij,sbjh->sbih", lower_mask.astype(jnp.float32), grouped, precision=PRECISE)
    group_total = within[:, :, -1, :]
    through = jnp.cumsum(group_total, axis=1)
    before = through - group_total
    return (lower_mask, within, group_total, through, before)


def group_core(values, step_size, log_decay, b_state, c_state, skip_gain):
    seq_count, tokens, width = values.shape
    head_count = step_size.shape[2]
    head_dim = width // head_count
    blocks = tokens // GROUP
    lower_mask, within, group_total, through, before = running_decay(log_decay)
    head_values = values.reshape(seq_count, blocks, GROUP, head_count, head_dim)
    step_blocks = step_size.reshape(seq_count, blocks, GROUP, head_count)
    b_blocks = b_state.reshape(seq_count, blocks, GROUP, -1)
    c_blocks = c_state.reshape(seq_count, blocks, GROUP, -1)
    decay_rows = within.transpose(0, 1, 3, 2)
    log_gaps = decay_rows[..., :, None] - decay_rows[..., None, :]
    decay_mat = jnp.where(lower_mask, jnp.exp(jnp.where(lower_mask, log_gaps, 0.0)), 0.0)
    scores = jnp.einsum("sbin,sbjn->sbij", c_blocks, b_blocks, precision=PRECISE)
    weighted = scores[:, :, None] * decay_mat * step_blocks.transpose(0, 1, 3, 2)[:, :, :, None, :]
    intra_out = jnp.einsum("sbhij,sbjhp->sbihp", weighted, head_values, precision=PRECISE)
    to_end = jnp.exp(group_total[:, :, None, :] - within) * step_blocks
    states = jnp.einsum("sbjh,sbjhp,sbjn->sbhpn", to_end, head_values, b_blocks, precision=PRECISE)
    later_at = lax.broadcasted_iota(jnp.int32, (blocks, blocks), 0)
    earlier_at = lax.broadcasted_iota(jnp.int32, (blocks, blocks), 1)
    earlier_mask = (later_at > earlier_at)[None, :, :, None]
    carry_gap = before[:, :, None, :] - through[:, None, :, :]
    carry_factor = jnp.where(earlier_mask, jnp.exp(jnp.where(earlier_mask, carry_gap, 0.0)), 0.0)
    entering = jnp.einsum("skmh,smhpn->skhpn", carry_factor, states, precision=PRECISE)
    inter_out = (
        jnp.einsum("sbin,sbhpn->sbihp", c_blocks, entering, precision=PRECISE)
        * jnp.exp(within)[..., None]
    )
    output = intra_out + inter_out + skip_gain[:, None] * head_values
    end_gap = through - through
    summary = jnp.einsum("sbh,sbhpn->shpn", jnp.exp(end_gap), states, precision=PRECISE)
    decay_all = jnp.exp(through[:, -1, :])
    return (output.reshape(seq_count, tokens, width), decay_all, summary)


def entry_term(entry_state, log_decay, c_state):
    seq_count, tokens, head_count = log_decay.shape
    blocks = tokens // GROUP
    _, within, _, _, before = running_decay(log_decay)
    reach = jnp.exp(within + before[:, :, None, :])
    c_blocks = c_state.reshape(seq_count, blocks, GROUP, -1)
    result = (
        jnp.einsum("sbin,shpn->sbihp", c_blocks, entry_state, precision=PRECISE) * reach[..., None]
    )
    return result.reshape(seq_count, tokens, -1)


def full_mixer(values, step_size, log_decay, b_state, c_state, skip_gain, entry_state):
    base_out, decay_all, summary = group_core(
        values, step_size, log_decay, b_state, c_state, skip_gain
    )
    output = base_out + entry_term(entry_state, log_decay, c_state)
    leaving = decay_all[..., None, None] * entry_state + summary
    return (output, leaving)


def gram_strips(rows):
    size = rows.shape[1]
    block = min(size, 256)
    return [
        jnp.einsum("ri,rj->ij", rows[:, at : at + block], rows[:, at:], precision=PRECISE)
        for at in range(0, size, block)
    ]


def orthogonal_kernel(arrays, strip_counts, *refs):

    grams = []
    for strips in strip_counts:
        grams.append(refs[:strips])
        refs = refs[strips:]
    rows, outs, scratch = refs[:arrays], refs[arrays : 2 * arrays], refs[2 * arrays :]
    work = [scratch[8 * j : 8 * j + 8] for j in range(arrays)]
    for j in range(arrays):
        whole = work[j][0]
        block = grams[j][0].shape[0]
        spots = [slice(at * block, (at + 1) * block) for at in range(len(grams[j]))]
        across = lax.broadcasted_iota(jnp.int32, (block, block), 0)
        down = lax.broadcasted_iota(jnp.int32, (block, block), 1)
        total = jnp.zeros((1, 1), jnp.float32)
        for strip in grams[j]:
            diagonal = jnp.where(across == down, strip[:, :block], 0.0)
            total += jnp.sum(jnp.sum(diagonal, axis=0, keepdims=True), axis=1, keepdims=True)
        factor = 1.0 / (jnp.sqrt(total) + 1e-07)
        square = factor * factor
        for i, strip in enumerate(grams[j]):
            for k in range(i, len(spots)):
                piece = strip[:, (k - i) * block : (k - i + 1) * block] * square
                whole[spots[i], spots[k]] = piece
                if i != k:
                    whole[spots[k], spots[i]] = piece.T
        outs[j][...] = rows[j][...] * factor

    def split_whole(j, at):
        whole, high, low = work[j][0], work[j][1], work[j][2]
        high[at, :], low[at, :] = halves(whole[at, :])

    def sweep(last):
        strips = []
        for j in range(arrays):
            size = rows[j].shape[1]
            strip = min(size, 256)
            strips.append([slice(s, s + strip) for s in range(0, size, strip)])
        for j in range(arrays):
            for at in strips[j]:
                split_whole(j, at)
        for j in range(arrays):
            whole, high, low, poly_h, poly_l, _, _, _ = work[j]
            for at in strips[j]:
                poly = QUINTIC_B * whole[at, :] + QUINTIC_C * three_pass(
                    (high[at, :], low[at, :]), (high[...], low[...])
                )
                poly_h[at, :], poly_l[at, :] = halves(poly)
        for j in range(arrays):
            poly = (work[j][3][...], work[j][4][...])
            value = outs[j][...]
            outs[j][...] = QUINTIC_A * value + three_pass(halves(value), poly)
        if last:
            return
        for j in range(arrays):
            whole, high, low, poly_h, poly_l, half, half_h, half_l = work[j]
            for at in strips[j]:
                value = QUINTIC_A * whole[at, :] + three_pass(
                    (poly_h[at, :], poly_l[at, :]), (high[...], low[...])
                )
                half[at, :] = value
                half_h[at, :], half_l[at, :] = halves(value)
        for j in range(arrays):
            whole, _, _, poly_h, poly_l, half, half_h, half_l = work[j]
            for at in strips[j]:
                whole[at, :] = QUINTIC_A * half[at, :] + three_pass(
                    (half_h[at, :], half_l[at, :]), (poly_h[...], poly_l[...])
                )

    def body(_, carry):
        sweep(False)
        return carry

    lax.fori_loop(0, SWEEPS - 1, body, 0)
    sweep(True)


def orthogonal_rows(pairs, name):
    arrays = len(pairs)
    scratch = []
    flops = 0
    for _, rows in pairs:
        size = rows.shape[1]
        full, narrow = pltpu.VMEM((size, size), jnp.float32), pltpu.VMEM((size, size), jnp.bfloat16)
        scratch += [full, narrow, narrow, narrow, narrow, full, narrow, narrow]
        flops += 6 * (13 * size**3 + 5 * rows.shape[0] * size**2)
    return pl.pallas_call(
        functools.partial(orthogonal_kernel, arrays, [len(strips) for strips, _ in pairs]),
        out_shape=[jax.ShapeDtypeStruct(rows.shape, jnp.float32) for _, rows in pairs],
        in_specs=[pl.BlockSpec(memory_space=pltpu.VMEM)]
        * (arrays + sum(len(strips) for strips, _ in pairs)),
        out_specs=[pl.BlockSpec(memory_space=pltpu.VMEM)] * arrays,
        scratch_shapes=scratch,
        cost_estimate=pl.CostEstimate(flops=flops, bytes_accessed=0, transcendentals=0),
        name=name,
    )(*[strip for strips, _ in pairs for strip in strips], *[rows for _, rows in pairs])


def on_device(
    block_input,
    cotangent,
    gate_proj,
    value_proj,
    bc_proj,
    step_proj,
    out_proj,
    in_gain,
    conv_value,
    conv_bc,
    head_params,
    out_gain,
    m_gate,
    m_value,
    m_bc,
    m_step,
    m_out,
    m_ingain,
    m_convvalue,
    m_convbc,
    m_head,
    m_outgain,
):
    head_count = lax.axis_size("head")
    head_index = lax.axis_index("head")
    seq_count, tokens, _ = block_input.shape
    row_count = gate_proj.shape[0]
    inner_width = gate_proj.shape[1]
    local_heads = step_proj.shape[1]
    bc_width = 2 * STATE // head_count
    model_part = D // head_count
    side_width = -(-(bc_width + local_heads) // LANES) * LANES
    bc_cols_mine = lax.dynamic_slice_in_dim(bc_proj, head_index * bc_width, bc_width, 1)
    side_mine = jnp.concatenate(
        [
            value_proj,
            bc_cols_mine,
            step_proj,
            jnp.zeros((row_count, side_width - bc_width - local_heads), jnp.float32),
        ],
        axis=1,
    )
    conv_mine = lax.dynamic_slice_in_dim(conv_value, head_index * inner_width, inner_width, 1)
    gain_mine = lax.dynamic_slice_in_dim(out_gain, head_index * inner_width, inner_width, 0)
    head_mine = lax.dynamic_slice_in_dim(head_params, head_index * local_heads, local_heads, 1)
    bc_taps = lax.dynamic_slice_in_dim(conv_bc, head_index * bc_width, bc_width, 1)
    inv_rms = lax.rsqrt(jnp.mean(block_input * block_input, axis=-1, keepdims=True) + EPSILON)
    normed = block_input * inv_rms * in_gain
    normed_turned = normed[0].T
    cotangent_turned = cotangent[0].T
    mixed_full, all_pre = ring_gather((side_mine,), (normed_turned,), "seq", 0)
    all_pre = all_pre[None]
    mixed_width = inner_width + bc_width
    mixed_pre = all_pre[..., :mixed_width]
    step_pre = all_pre[..., mixed_width : mixed_width + local_heads]
    conv_taps = jnp.concatenate([conv_mine, bc_taps], axis=-1)
    edge_rows = from_behind(mixed_pre[:, tokens - (CONV - 1) :, :], "seq", 1)
    padded = jnp.concatenate([edge_rows, mixed_pre], axis=1)
    conv_out = conv_taps[CONV] + sum(
        (conv_taps[offset] * padded[:, offset : offset + tokens, :] for offset in range(CONV))
    )
    activated = jax.nn.silu(conv_out)
    values = activated[..., :inner_width]
    bc_all = lax.all_gather(activated[..., inner_width:], "head", axis=2, tiled=True)
    b_state = bc_all[..., :STATE]
    c_state = bc_all[..., STATE:]
    decay_rate = jnp.exp(head_mine[0])
    skip_gain = head_mine[1]
    step_arg = step_pre + head_mine[2]
    step_size = jax.nn.softplus(step_arg)
    log_decay = -decay_rate * step_size
    base_out, decay_all, summary = group_core(
        values, step_size, log_decay, b_state, c_state, skip_gain
    )
    state_shape = summary.shape
    state_rows = (-1, state_shape[-1])
    decay_rows = jnp.broadcast_to(decay_all[..., None, None], state_shape).reshape(state_rows)
    gate_full, out_full, gate_pre, grad_normout, entry_rows = ring_gather(
        (gate_proj, out_proj.T),
        (normed_turned, cotangent_turned),
        "seq",
        1,
        (summary.reshape(state_rows), decay_rows, False),
    )
    gate_pre, grad_normout = gate_pre[None], grad_normout[None]
    entry_state = entry_rows.reshape(state_shape)
    mixer_out = base_out + entry_term(entry_state, log_decay, c_state)
    gate_act = jax.nn.silu(gate_pre)
    gated = mixer_out * gate_act
    square_part = jnp.sum(gated * gated, axis=-1, keepdims=True)
    out_part = back_project(gated * gain_mine, out_full)
    out_sum = lax.psum_scatter(out_part, "head", scatter_dimension=2, tiled=True)
    scaled = grad_normout * gain_mine
    dot_part = jnp.sum(scaled * gated, axis=-1, keepdims=True)
    both = lax.psum(jnp.concatenate([square_part, dot_part], axis=-1), "head")
    square_sum, dot_total = both[..., :1], both[..., 1:]
    gate_rms = lax.rsqrt(square_sum / DI + EPSILON)
    input_mine = lax.dynamic_slice_in_dim(block_input, head_index * model_part, model_part, 2)
    cotangent_mine = lax.dynamic_slice_in_dim(cotangent, head_index * model_part, model_part, 2)
    normed_out = gated * gate_rms * gain_mine
    grad_outgain_mine = jnp.sum(grad_normout * gated * gate_rms, axis=(0, 1))
    grad_gated = gate_rms * scaled - gate_rms**3 * gated * dot_total / DI
    grad_mixer = grad_gated * gate_act
    grad_gate_pre = grad_gated * mixer_out * silu_grad(gate_pre)
    _, entry_back = jax.vjp(lambda entering: entry_term(entering, log_decay, c_state), entry_state)
    direct = entry_back(grad_mixer)[0]
    grad_out_rows, grad_gate, leave_rows = ring_scatter(
        ((cotangent_turned, normed_out[0]), (normed_turned, grad_gate_pre[0])),
        "seq",
        2,
        (direct.reshape(state_rows), decay_rows, True),
    )
    leave_rows, out_sum = lax.optimization_barrier((leave_rows, out_sum))
    block_output = input_mine + gate_rms * out_sum
    next_out_rows = MOMENTUM_KEEP * m_out.T + grad_out_rows
    next_gate = MOMENTUM_KEEP * m_gate + grad_gate
    strips = len(gram_strips(next_gate))
    early = gram_strips(next_out_rows) + gram_strips(next_gate)
    early, leave_rows = lax.optimization_barrier((early, leave_rows))
    early = lax.psum(early, "seq")
    leave_grad = leave_rows.reshape(state_shape)
    _, mixer_back = jax.vjp(
        full_mixer, values, step_size, log_decay, b_state, c_state, skip_gain, entry_state
    )
    grad_values, grad_stepsize, grad_logdecay, grad_b, grad_c, grad_skip, _ = mixer_back(
        (grad_mixer, leave_grad)
    )
    grad_step_total = grad_stepsize - grad_logdecay * decay_rate
    grad_alog = jnp.sum(grad_logdecay * log_decay, axis=(0, 1))
    grad_step_pre = grad_step_total * jax.nn.sigmoid(step_arg)
    grad_bias = jnp.sum(grad_step_pre, axis=(0, 1))
    grad_bc_all = jnp.concatenate([grad_b, grad_c], axis=-1)
    grad_bc_act = direct_scatter(
        grad_bc_all[0].T.reshape(head_count, bc_width, tokens), "head", 4
    ).T[None]
    grad_conv = jnp.concatenate([grad_values, grad_bc_act], axis=-1) * silu_grad(conv_out)
    grad_taps = jnp.stack(
        [
            jnp.sum(grad_conv * padded[:, offset : offset + tokens, :], axis=(0, 1))
            for offset in range(CONV)
        ]
        + [jnp.sum(grad_conv, axis=(0, 1))]
    )
    grad_padded = sum(
        (
            jnp.pad(conv_taps[offset] * grad_conv, ((0, 0), (offset, CONV - 1 - offset), (0, 0)))
            for offset in range(CONV)
        )
    )
    edge_back = from_behind(grad_padded[:, : CONV - 1, :], "seq", -1)
    grad_mixed = grad_padded[:, CONV - 1 :, :] + jnp.pad(
        edge_back, ((0, 0), (tokens - (CONV - 1), 0), (0, 0))
    )
    grad_all_pre = jnp.concatenate(
        [
            grad_mixed,
            grad_step_pre,
            jnp.zeros((seq_count, tokens, side_width - bc_width - local_heads), jnp.float32),
        ],
        axis=-1,
    )
    grad_normed = back_project(grad_gate_pre, gate_full) + back_project(grad_all_pre, mixed_full)
    stat_part = jnp.sum(grad_normed * in_gain * block_input, axis=-1, keepdims=True)
    grad_ingain_part = jnp.sum(grad_normed * block_input * inv_rms, axis=(0, 1))
    (grad_mixed_rows,) = ring_scatter(((normed_turned, grad_all_pre[0]),), "seq", 3)
    grad_value = grad_mixed_rows[:, :inner_width]
    grad_bc = lax.all_gather(
        grad_mixed_rows[:, inner_width:mixed_width], "head", axis=1, tiled=True
    )
    grad_step = grad_mixed_rows[:, mixed_width : mixed_width + local_heads]
    grad_out = grad_out_rows.T
    next_value = MOMENTUM_KEEP * m_value + grad_value
    next_bc = MOMENTUM_KEEP * m_bc + grad_bc
    next_step = MOMENTUM_KEEP * m_step + grad_step
    next_out = MOMENTUM_KEEP * m_out + grad_out
    pieces = (
        grad_ingain_part,
        grad_taps.reshape(-1),
        grad_alog,
        grad_skip,
        grad_bias,
        grad_outgain_mine,
    )
    flat = jnp.concatenate(pieces)
    flat_rows = -(-flat.shape[0] // (16 * STATE)) * 8
    flat = jnp.pad(flat, (0, flat_rows * 2 * STATE - flat.shape[0])).reshape(flat_rows, 2 * STATE)
    side = 2 * STATE
    late_value, early = lax.optimization_barrier((next_value, early))
    out_gram, gate_gram = early[:strips], early[strips:]
    (step_gram,) = gram_strips(next_step)
    step_gram = jnp.pad(step_gram, ((0, -local_heads % 8), (0, side - local_heads)))
    late = lax.psum(
        gram_strips(late_value)
        + [jnp.concatenate(gram_strips(next_bc) + [step_gram, flat], axis=0)],
        "seq",
    )
    value_gram, side_gram = late[:-1], late[-1]
    flat = side_gram[side + step_gram.shape[0] :]
    step_gram = jnp.pad(
        side_gram[side : side + step_gram.shape[0], :LANES],
        ((0, LANES - step_gram.shape[0]), (0, 0)),
    )
    flat = lax.all_gather(flat, "head").reshape(head_count, flat_rows * 2 * STATE)
    parts = []
    start = 0
    for piece in pieces:
        parts.append(flat[:, start : start + piece.shape[0]])
        start += piece.shape[0]
    grad_ingain = jnp.sum(parts[0], axis=0)
    taps_all = parts[1].reshape(head_count, CONV + 1, mixed_width)
    grad_convvalue = taps_all[:, :, :inner_width].transpose(1, 0, 2).reshape(CONV + 1, DI)
    grad_convbc = taps_all[:, :, inner_width:].transpose(1, 0, 2).reshape(CONV + 1, 2 * STATE)
    grad_head = jnp.stack([parts[2].reshape(H), parts[3].reshape(H), parts[4].reshape(H)])
    grad_outgain = parts[5].reshape(DI)
    next_ingain = MOMENTUM_KEEP * m_ingain + grad_ingain
    next_convvalue = MOMENTUM_KEEP * m_convvalue + grad_convvalue
    next_convbc = MOMENTUM_KEEP * m_convbc + grad_convbc
    next_head = MOMENTUM_KEEP * m_head + grad_head
    next_outgain = MOMENTUM_KEEP * m_outgain + grad_outgain
    update_out, update_gate = orthogonal_rows(
        ((out_gram, next_out_rows), (gate_gram, next_gate)), "ortho_first"
    )
    grad_normed, stat_part, side_gram = lax.optimization_barrier(
        (grad_normed, stat_part, side_gram)
    )
    update_out = update_out.T
    normed_grad_mine = lax.psum_scatter(grad_normed, "head", scatter_dimension=2, tiled=True)
    stat_total = lax.psum(stat_part, "head")
    gain_part = lax.dynamic_slice_in_dim(in_gain, head_index * model_part, model_part, 0)
    input_grad = (
        cotangent_mine
        + inv_rms * gain_part * normed_grad_mine
        - inv_rms**3 * input_mine * stat_total / D
    )
    update_value, update_bc, update_step = orthogonal_rows(
        (
            (value_gram, next_value),
            ([side_gram[:side]], next_bc),
            ([step_gram], jnp.pad(next_step, ((0, 0), (0, LANES - local_heads)))),
        ),
        "ortho_last",
    )
    update_step = update_step[:, :local_heads]
    update_scale = MATRIX_RATE * MUON_SCALE * math.sqrt(D)
    new_gate = gate_proj - update_scale * update_gate
    new_value = value_proj - update_scale * update_value
    new_bc = bc_proj - update_scale * update_bc
    new_step = step_proj - update_scale * update_step
    new_out = out_proj - update_scale * update_out
    new_ingain = in_gain - VECTOR_RATE * next_ingain
    new_convvalue = conv_value - VECTOR_RATE * next_convvalue
    new_convbc = conv_bc - VECTOR_RATE * next_convbc
    new_head = head_params - VECTOR_RATE * next_head
    new_outgain = out_gain - VECTOR_RATE * next_outgain
    return (
        block_output,
        input_grad,
        grad_gate,
        grad_value,
        grad_bc,
        grad_step,
        grad_out,
        grad_ingain,
        grad_convvalue,
        grad_convbc,
        grad_head,
        grad_outgain,
        new_gate,
        new_value,
        new_bc,
        new_step,
        new_out,
        new_ingain,
        new_convvalue,
        new_convbc,
        new_head,
        new_outgain,
        next_gate,
        next_value,
        next_bc,
        next_step,
        next_out,
        next_ingain,
        next_convvalue,
        next_convbc,
        next_head,
        next_outgain,
    )


def solution(mesh):
    in_specs = (
        P(None, "seq", None),
        P(None, "seq", None),
        P("seq", "head"),
        P("seq", "head"),
        P("seq", None),
        P("seq", "head"),
        P("head", "seq"),
        P(),
        P(),
        P(),
        P(),
        P(),
        P("seq", "head"),
        P("seq", "head"),
        P("seq", None),
        P("seq", "head"),
        P("head", "seq"),
        P(),
        P(),
        P(),
        P(),
        P(),
    )
    out_specs = (
        P(None, "seq", "head"),
        P(None, "seq", "head"),
        P("seq", "head"),
        P("seq", "head"),
        P("seq", None),
        P("seq", "head"),
        P("head", "seq"),
        P(),
        P(),
        P(),
        P(),
        P(),
        P("seq", "head"),
        P("seq", "head"),
        P("seq", None),
        P("seq", "head"),
        P("head", "seq"),
        P(),
        P(),
        P(),
        P(),
        P(),
        P("seq", "head"),
        P("seq", "head"),
        P("seq", None),
        P("seq", "head"),
        P("head", "seq"),
        P(),
        P(),
        P(),
        P(),
        P(),
    )
    return jax.shard_map(
        on_device, mesh=mesh, in_specs=in_specs, out_specs=out_specs, check_vma=False
    )
```
